256 devices in a mesh: groups: 4 (over x, y), blk: 32 (over z), rows: 2 (over core).
Axes of the slice: x: 2, y: 2, z: 32, core: 2. Of those that a mesh axis runs over, the one named last changes fastest.
The devices are a block of a 4x8x32 slice.
Arguments:
- features: bfloat16 [16, 16, 1024, 512], P('groups', 'rows', 'blk'), parts along dimension 0, may hold values from -60 to 60
- gain_in: float32 [512], replicated, may hold values from 0.25 to 1.75
- shift_in: float32 [512], replicated, may hold values from -3 to 3
- conv_first: bfloat16 [3, 3, 512, 256], replicated, may hold values from -0.09375 to 0.09375
- bias_first: float32 [256], replicated, may hold values from -3 to 3
- short_weight: bfloat16 [512, 256], replicated, may hold values from -0.25 to 0.25
- short_bias: float32 [256], replicated, may hold values from -3 to 3
- gains_rest: float32 [5, 256], replicated, may hold values from 0.25 to 1.75
- shifts_rest: float32 [5, 256], replicated, may hold values from -3 to 3
- convs_rest: bfloat16 [5, 3, 3, 256, 256], replicated, may hold values from -0.125 to 0.125
- biases_rest: float32 [5, 256], replicated, may hold values from -3 to 3
Outputs:
- decoded: bfloat16 [16, 16, 1024, 256], P('groups', 'rows', 'blk'), parts along dimension 0
The draws below stay inside these ranges and needn't reach their ends.
There are 4 independent parts, one for each index of `groups`. The reference program is written for one: setup_inputs(seed, part) draws one part's arguments, and reference() takes and returns one part's arrays. A program takes and returns all parts, laid end to end along the dimension named above; an argument that names none is the same for every part. Nothing has to cross between parts.
All inputs are finite; a program needn't handle non-finite values.
Results may differ from the reference program's by a relative error of at most 0.0065.
Values may be sent and summed in bfloat16 or wider, within the bound.
A program may use at most 128 MiB of HBM per device.

```python
import math
import jax
import jax.numpy as jnp
from jax import lax

CH_IN = 512
CH = 256
GROUPS = 32
RESNETS = 3
IMAGES = 4
ROWS_ALL = 16
COLS_ALL = 1024


def draw_features(key, part):
    keys = jax.random.split(jax.random.fold_in(key, 17), 5)
    shape = (IMAGES, ROWS_ALL, COLS_ALL, CH_IN)
    base = jax.random.normal(keys[0], shape, jnp.float32)
    rise = math.log(6.0)
    chan_scale = jnp.exp(jax.random.uniform(keys[1], (CH_IN,), jnp.float32, 0.0, math.log(10.0)))
    chan_mean = 0.8 * jax.random.normal(keys[2], (CH_IN,), jnp.float32)
    position = jnp.arange(COLS_ALL, dtype=jnp.float32) / COLS_ALL
    column_scale = jnp.exp(rise * position + jax.random.uniform(keys[3], (COLS_ALL,), jnp.float32, 0.0, math.log(2.0)))
    row_scale = jnp.exp(jax.random.uniform(keys[4], (ROWS_ALL,), jnp.float32, 0.0, math.log(2.0)))
    values = (base + chan_mean) * chan_scale * column_scale[None, None, :, None] * row_scale[None, :, None, None] * 0.15
    return jnp.clip(values, -60.0, 60.0).astype(jnp.bfloat16)


def gaussian(key, shape, width, most, kind=jnp.bfloat16):
    values = width * jax.random.normal(key, shape, jnp.float32)
    return jnp.clip(values, min=-most, max=most).astype(kind)


def setup_inputs(seed: int = 0, part: int = 0) -> dict:
    key_of = jax.random.split(jax.random.key(seed), 12)
    part_keys = jax.random.split(jax.random.fold_in(key_of[11], part), 12)
    features = draw_features(jax.random.fold_in(jax.random.fold_in(key_of[11], part), 71), part)
    gain_in = jnp.clip(1.0 + 0.15 * jax.random.normal(key_of[1], (CH_IN,), jnp.float32), 0.25, 1.75)
    shift_in = gaussian(key_of[2], (CH_IN,), 0.4, 3.0, jnp.float32)
    conv_first = gaussian(key_of[3], (3, 3, CH_IN, CH), (9 * CH_IN) ** -0.5, 0.09375)
    bias_first = gaussian(key_of[4], (CH,), 0.4, 3.0, jnp.float32)
    short_weight = gaussian(key_of[5], (CH_IN, CH), CH_IN ** -0.5, 0.25)
    short_bias = gaussian(key_of[6], (CH,), 0.4, 3.0, jnp.float32)
    gains_rest = jnp.clip(1.0 + 0.15 * jax.random.normal(key_of[7], (2 * RESNETS - 1, CH), jnp.float32), 0.25, 1.75)
    shifts_rest = gaussian(key_of[8], (2 * RESNETS - 1, CH), 0.4, 3.0, jnp.float32)
    convs_rest = gaussian(key_of[9], (2 * RESNETS - 1, 3, 3, CH, CH), (9 * CH) ** -0.5, 0.125)
    biases_rest = gaussian(key_of[10], (2 * RESNETS - 1, CH), 0.4, 3.0, jnp.float32)
    return dict(features=features, gain_in=gain_in, shift_in=shift_in, conv_first=conv_first, bias_first=bias_first, short_weight=short_weight, short_bias=short_bias, gains_rest=gains_rest, shifts_rest=shifts_rest, convs_rest=convs_rest, biases_rest=biases_rest)


EPS = 1e-06

def norm_act(values, gain, shift):
    count = values.shape[3] // GROUPS
    grouped = values.reshape(values.shape[0], values.shape[1], values.shape[2], GROUPS, count)
    center = lax.optimization_barrier(jnp.mean(grouped, axis=(1, 2, 4), keepdims=True))
    spread = lax.optimization_barrier(jnp.mean(jnp.square(grouped - center), axis=(1, 2, 4), keepdims=True))
    scaled = ((grouped - center) * lax.rsqrt(spread + EPS)).reshape(values.shape) * gain + shift
    return (scaled * jax.nn.sigmoid(scaled)).astype(jnp.bfloat16)

def convolve(field, weight, bias):
    wrapped = jnp.concatenate([field[:, :, -1:], field, field[:, :, :1]], axis=2)
    padded = jnp.pad(wrapped, ((0, 0), (1, 1), (0, 0), (0, 0)))
    result = lax.conv_general_dilated(padded.astype(jnp.float32), weight.astype(jnp.float32), (1, 1), 'VALID', dimension_numbers=('NHWC', 'HWIO', 'NHWC'), precision=lax.Precision.HIGHEST)
    return result + bias

def reference(features, gain_in, shift_in, conv_first, bias_first, short_weight, short_bias, gains_rest, shifts_rest, convs_rest, biases_rest):
    stream = features
    for block in range(RESNETS):
        if block == 0:
            first = (gain_in, shift_in, conv_first, bias_first)
        else:
            first = (gains_rest[2 * block - 1], shifts_rest[2 * block - 1], convs_rest[2 * block - 1], biases_rest[2 * block - 1])
        second = (gains_rest[2 * block], shifts_rest[2 * block], convs_rest[2 * block], biases_rest[2 * block])
        active = norm_act(stream.astype(jnp.float32), first[0], first[1])
        inner = convolve(active, first[2], first[3]).astype(jnp.bfloat16)
        active_two = norm_act(inner.astype(jnp.float32), second[0], second[1])
        branch = convolve(active_two, second[2], second[3])
        if block == 0:
            flat = stream.reshape(-1, stream.shape[3])
            skip = jnp.dot(flat, short_weight, preferred_element_type=jnp.float32) + short_bias
            skip = skip.reshape(stream.shape[0], stream.shape[1], stream.shape[2], short_weight.shape[1])
        else:
            skip = stream.astype(jnp.float32)
        stream = (skip + branch).astype(jnp.bfloat16)
    return stream
```

```python
import functools

import jax
import jax.numpy as jnp
from jax import lax
from jax.experimental import pallas as pl
from jax.experimental.pallas import tpu as pltpu
from jax.sharding import PartitionSpec as P

GROUPS = 32
RESNETS = 3
EPS = 1e-06
LANES = 128
MESH = pl.DeviceIdType.MESH
F32 = jnp.float32
BF16 = jnp.bfloat16


def iota(shape, dim):
    return lax.broadcasted_iota(jnp.int32, shape, dim)


def three_parts(values, part):
    high = values.astype(BF16)
    rest = values - high.astype(F32)
    middle = rest.astype(BF16)
    low = (rest - middle.astype(F32)).astype(BF16)
    picked = jnp.where(part == 0, high.astype(F32), jnp.where(part == 1, middle.astype(F32), low.astype(F32)))
    return jnp.where(part < 3, picked, 0.0).astype(BF16)


def kernel(
    nblk,
    nrow,
    halves,
    x_hbm,
    gain_in,
    shift_in,
    w1_hbm,
    bias_first,
    sw_hbm,
    short_bias,
    gains,
    shifts,
    wr_hbm,
    biases,
    out_hbm,
    xv,
    w1,
    wr,
    sw,
    v0,
    vs,
    stream,
    a1,
    a2,
    outv,
    col_s1,
    col_r1,
    row_r1,
    cor_s1,
    cor_r1,
    col_s2,
    col_r2,
    row_r2,
    cor_s2,
    cor_r2,
    stat_s,
    stat_r,
    x_sem,
    w_sem,
    out_sem,
    stat_ssem,
    stat_rsem,
    halo_ssem,
    colr_sem,
    rowr_sem,
    corr_sem,
):
    images, height, width, _ = xv.shape
    per = images // halves
    slots = 2 * per
    pixels = height * width
    z = lax.axis_index("blk")
    c = lax.axis_index("rows")
    oc = 1 - c
    right = lax.rem(z + 1, nblk)
    left = lax.rem(z + nblk - 1, nblk)
    me = z * nrow + c
    edge = (height - 1) * (1 - c)
    halo_row = (height + 1) * (1 - c)
    zero_row = (height + 1) * c

    x_copies = [pltpu.make_async_copy(x_hbm.at[i], xv.at[i], x_sem.at[i]) for i in range(images)]
    for copy in x_copies:
        copy.start()
    w_copies = [
        pltpu.make_async_copy(sw_hbm, sw, w_sem.at[0]),
        pltpu.make_async_copy(w1_hbm, w1, w_sem.at[1]),
    ] + [pltpu.make_async_copy(wr_hbm.at[i], wr.at[i], w_sem.at[2 + i]) for i in range(wr_hbm.shape[0])]
    for copy in w_copies:
        copy.start()

    barrier = pltpu.get_barrier_semaphore()

    def greet(d, carry):
        zz = lax.rem(z + d, nblk)
        pl.semaphore_signal(barrier, 1, device_id={"blk": zz, "rows": oc}, device_id_type=MESH)

        @pl.when(d > 0)
        def _():
            pl.semaphore_signal(barrier, 1, device_id={"blk": zz, "rows": c}, device_id_type=MESH)

        return carry

    lax.fori_loop(0, nblk, greet, 0)

    for a in (a1, a2):
        for i in range(images):
            a[i, zero_row] = jnp.zeros(a.shape[2:], BF16)

    def gather_matrix(channels):
        return (iota((channels, LANES), 0) // (channels // GROUPS) == iota((channels, LANES), 1) % GROUPS).astype(F32).astype(BF16)

    def spread_matrix(channels):
        return (iota((LANES, channels), 0) % GROUPS == iota((LANES, channels), 1) // (channels // GROUPS)).astype(F32).astype(BF16)

    def local_stats(k, h, rows):
        channels = rows[0].shape[1]
        which = iota((16, channels), 0)
        base = jnp.broadcast_to(rows[0], (16, channels))
        for j in range(1, slots):
            base = jnp.where(which % slots == j, rows[j], base)
        lhs = three_parts(base, which // slots)
        dots = jnp.dot(lhs, gather_matrix(channels), preferred_element_type=F32)
        slot_of_row = iota((16, LANES), 0) % slots
        slot_of_lane = iota((16, LANES), 1) // GROUPS
        packed = jnp.sum(jnp.where(slot_of_row == slot_of_lane, dots, 0.0), axis=0, keepdims=True)
        stat_s[k, h] = jnp.broadcast_to(packed, (8, LANES))
        stat_r[k, h, pl.ds(me, 1)] = packed

    def send_stats(k, h):
        source = stat_s.at[k, h, pl.ds(0, 1)]
        target = stat_r.at[k, h, pl.ds(me, 1)]

        def to(zz, cc):
            pltpu.make_async_remote_copy(
                source, target, stat_ssem.at[k, h], stat_rsem.at[k, h],
                device_id={"blk": zz, "rows": cc}, device_id_type=MESH,
            ).start()

        half_way = nblk // 2
        to(lax.rem(z + half_way, nblk), oc)
        to(lax.rem(z + half_way, nblk), c)

        def step(i, carry):
            d = half_way - 1 - i
            for zz in (lax.rem(z + d, nblk), lax.rem(z + nblk - d, nblk)):
                to(zz, oc)
                to(zz, c)
            return carry

        lax.fori_loop(0, half_way - 1, step, 0)
        to(z, oc)

    def wait_stats(k, h):
        count = nblk * nrow - 1
        copy = pltpu.make_async_remote_copy(
            stat_r.at[k, h, pl.ds(0, count)], stat_r.at[k, h, pl.ds(0, count)],
            stat_ssem.at[k, h], stat_rsem.at[k, h], device_id={"rows": oc}, device_id_type=MESH,
        )
        copy.wait_send()
        copy.wait_recv()

    def scales(k, h, channels, gain, shift):
        count = pixels * nblk * nrow * (channels // GROUPS)
        total = jnp.sum(stat_r[k, h], axis=0, keepdims=True) / count
        total = jnp.broadcast_to(total, (16, LANES))
        center = pltpu.roll(total, GROUPS, 1)
        spread = lax.rsqrt(jnp.maximum(total - center * center, 0.0) + EPS)
        slot_of_lane = iota((16, LANES), 1) // GROUPS
        stat = jnp.where(slot_of_lane % 2 == 1, spread, total)
        row = iota((16, LANES), 0)
        stat = jnp.where(slot_of_lane == row % slots, stat, 0.0)
        lhs = three_parts(stat, row // slots)
        dots = jnp.dot(lhs, spread_matrix(channels), preferred_element_type=F32)
        pick = lambda j: dots[j : j + 1] + dots[slots + j : slots + j + 1] + dots[2 * slots + j : 2 * slots + j + 1]
        result = []
        for i in range(per):
            a = pick(2 * i + 1) * gain
            result.append((0.5 * a, 0.5 * (shift - pick(2 * i) * a)))
        return result

    def activate(values, ab):
        half = values * ab[0] + ab[1]
        return half + half * jnp.tanh(half)

    class Halo:
        pass

    def halo_of(k):
        o = Halo()
        first = k == 0
        o.v = v0 if first else vs.at[k - 1]
        o.col_s = col_s1 if first else col_s2.at[k - 1]
        o.col_r = col_r1 if first else col_r2.at[k - 1]
        o.row_r = row_r1 if first else row_r2.at[k - 1]
        o.cor_s = cor_s1 if first else cor_s2.at[k - 1]
        o.cor_r = cor_r1 if first else cor_r2.at[k - 1]
        o.channels = o.v.shape[-1]
        return o

    def halo_copies(k, h):
        o = halo_of(k)
        copies = []
        for side, (near, blk) in enumerate(((0, right), (1, left))):
            copies.append(pltpu.make_async_remote_copy(
                o.col_s.at[h, side], o.col_r.at[h, side], halo_ssem.at[k, h, 2 * side], colr_sem.at[k, h, side],
                device_id={"blk": blk, "rows": c}, device_id_type=MESH))
            copies.append(pltpu.make_async_remote_copy(
                o.cor_s.at[h, side], o.cor_r.at[h, side], halo_ssem.at[k, h, 2 * side + 1], corr_sem.at[k, h, side],
                device_id={"blk": blk, "rows": oc}, device_id_type=MESH))
        copies.append(pltpu.make_async_remote_copy(
            o.v.at[pl.ds(h * per, per), pl.ds(edge * width, width)], o.row_r.at[h], halo_ssem.at[k, h, 4], rowr_sem.at[k, h],
            device_id={"rows": oc}, device_id_type=MESH))
        return copies

    def prepare_halo(k, h):
        o = halo_of(k)
        for side in range(2):
            q = width - 1 if side == 0 else 0
            cols = []
            corners = []
            for i in range(per):
                image = h * per + i
                which = iota((height, o.channels), 0)
                col = jnp.broadcast_to(o.v[image, pl.ds(q, 1), :], (height, o.channels))
                for r in range(1, height):
                    col = jnp.where(which == r, o.v[image, pl.ds(r * width + q, 1), :], col)
                cols.append(col)
                corners.append(o.v[image, pl.ds(edge * width + q, 1), :])
            o.col_s[h, side] = jnp.concatenate(cols, axis=0).astype(BF16)
            for i in range(per):
                o.cor_s[h, side, pl.ds(i, 1)] = corners[i]

    def emit(k, h, rows):
        local_stats(k, h, rows)
        send_stats(k, h)
        prepare_halo(k, h)
        for copy in halo_copies(k, h):
            copy.start()

    def load(k, h, a, gain, shift):
        o = halo_of(k)
        channels = o.channels
        wait_stats(k, h)
        factors = scales(k, h, channels, gain, shift)
        for copy in halo_copies(k, h):
            copy.wait()
        column = iota((width, channels), 0)

        def put(image, row, act, low, high):
            a[image, row, :, pl.ds(0, channels)] = jnp.where(column == 0, low, pltpu.roll(act, 1, 0)).astype(BF16)
            a[image, row, :, pl.ds(channels, channels)] = act.astype(BF16)
            a[image, row, :, pl.ds(2 * channels, channels)] = jnp.where(
                column == width - 1, high, pltpu.roll(act, width - 1, 0)).astype(BF16)

        for i in range(per):
            image = h * per + i
            ab = factors[i]
            sides = [activate(o.col_r[h, s, pl.ds(i * height, height)].astype(F32), ab) for s in range(2)]
            corner = [activate(o.cor_r[h, s, pl.ds(i, 1)], ab) for s in range(2)]
            for r in range(height):
                act = activate(o.v[image, pl.ds(r * width, width), :], ab)
                put(image, r + 1, act, sides[0][r : r + 1], sides[1][r : r + 1])
            act = activate(o.row_r[h, i], ab)
            put(image, halo_row, act, corner[0], corner[1])

    def convolve(a, image, weight):
        depth = a.shape[-1]
        total = None
        for d in range(3):
            lhs = a[image, d : d + height].reshape(pixels, depth)
            term = jnp.dot(lhs, weight[d].reshape(depth, weight.shape[-1]), preferred_element_type=F32)
            total = term if total is None else total + term
        return total

    def sums(values):
        return [jnp.sum(values, axis=0, keepdims=True), jnp.sum(values * values, axis=0, keepdims=True)]

    for h in range(halves):
        for i in range(per):
            x_copies[h * per + i].wait()
    rows0 = []
    for image in range(images):
        values = xv[image].reshape(pixels, xv.shape[-1]).astype(F32)
        v0[image] = values
        rows0.append(sums(values))
    pl.semaphore_wait(barrier, nblk * nrow - 1)
    for h in range(halves):
        emit(0, h, sum(rows0[h * per : (h + 1) * per], []))

    w_copies[0].wait()
    for image in range(images):
        stream[image] = jnp.dot(
            xv[image].reshape(pixels, xv.shape[-1]), sw[...], preferred_element_type=F32) + short_bias[...]

    last = 2 * RESNETS - 1
    for k in range(2 * RESNETS):
        if k == 0:
            a, gain, shift, weight, bias = a1, gain_in[...], shift_in[...], w1, bias_first[...]
        else:
            j = k - 1
            a, gain, shift, weight, bias = a2, gains[j : j + 1], shifts[j : j + 1], wr.at[j], biases[j : j + 1]
        for h in range(halves):
            load(k, h, a, gain, shift)
            if h == 0:
                w_copies[1 + k].wait()
            rows = []
            for i in range(per):
                image = h * per + i
                result = convolve(a, image, weight) + bias
                if k % 2 == 1:
                    result = result + stream[image]
                rounded = result.astype(BF16)
                if k == last:
                    outv[image] = rounded.reshape(height, width, rounded.shape[-1])
                else:
                    values = rounded.astype(F32)
                    vs[k, image] = values
                    if k % 2 == 1:
                        stream[image] = values
                    rows += sums(values)
            if k < last:
                emit(k + 1, h, rows)
            else:
                pltpu.make_async_copy(
                    outv.at[pl.ds(h * per, per)], out_hbm.at[pl.ds(h * per, per)], out_sem.at[h]).start()
    for h in range(halves):
        pltpu.make_async_copy(
            outv.at[pl.ds(h * per, per)], out_hbm.at[pl.ds(h * per, per)], out_sem.at[h]).wait()


def run(nblk, nrow, halves, *args):
    x = args[0]
    w1, wr = args[3], args[9]
    images, height, width, cin = x.shape
    ch = w1.shape[-1]
    per = images // halves
    stages = 2 * RESNETS
    anywhere = pl.BlockSpec(memory_space=pl.ANY)
    inside = pl.BlockSpec(memory_space=pltpu.VMEM)
    specs = [anywhere, inside, inside, anywhere, inside, anywhere, inside, inside, inside, anywhere, inside]
    fixed = list(args)
    for j in (1, 2, 4, 6):
        fixed[j] = args[j].reshape(1, -1)

    def halo_buffers(lead, channels):
        return [
            pltpu.VMEM((*lead, halves, 2, per * height, channels), BF16),
            pltpu.VMEM((*lead, halves, 2, per * height, channels), BF16),
            pltpu.VMEM((*lead, halves, per, width, channels), F32),
            pltpu.VMEM((*lead, halves, 2, 8, channels), F32),
            pltpu.VMEM((*lead, halves, 2, 8, channels), F32),
        ]

    return pl.pallas_call(
        functools.partial(kernel, nblk, nrow, halves),
        out_shape=jax.ShapeDtypeStruct((images, height, width, ch), BF16),
        in_specs=specs,
        out_specs=anywhere,
        scratch_shapes=[
            pltpu.VMEM(x.shape, BF16),
            pltpu.VMEM(w1.shape, BF16),
            pltpu.VMEM(wr.shape, BF16),
            pltpu.VMEM((cin, ch), BF16),
            pltpu.VMEM((images, height * width, cin), F32),
            pltpu.VMEM((stages - 1, images, height * width, ch), F32),
            pltpu.VMEM((images, height * width, ch), F32),
            pltpu.VMEM((images, height + 2, width, 3 * cin), BF16),
            pltpu.VMEM((images, height + 2, width, 3 * ch), BF16),
            pltpu.VMEM((images, height, width, ch), BF16),
            *halo_buffers((), cin),
            *halo_buffers((stages - 1,), ch),
            pltpu.VMEM((stages, halves, 8, LANES), F32),
            pltpu.VMEM((stages, halves, nblk * nrow, LANES), F32),
            pltpu.SemaphoreType.DMA((images,)),
            pltpu.SemaphoreType.DMA((1 + stages,)),
            pltpu.SemaphoreType.DMA((halves,)),
            pltpu.SemaphoreType.DMA((stages, halves)),
            pltpu.SemaphoreType.DMA((stages, halves)),
            pltpu.SemaphoreType.DMA((stages, halves, 5)),
            pltpu.SemaphoreType.DMA((stages, halves, 2)),
            pltpu.SemaphoreType.DMA((stages, halves)),
            pltpu.SemaphoreType.DMA((stages, halves, 2)),
        ],
        compiler_params=pltpu.CompilerParams(
            collective_id=0, has_side_effects=True, vmem_limit_bytes=60 * 1024 * 1024),
    )(*fixed)


def solution(mesh):
    placed = (P("groups", "rows", "blk", None),) + (P(),) * 10
    return jax.shard_map(
        functools.partial(run, mesh.shape["blk"], mesh.shape["rows"], 2),
        mesh=mesh,
        in_specs=placed,
        out_specs=P("groups", "rows", "blk", None),
        check_vma=False,
    )
```

```python
import functools

import jax
import jax.numpy as jnp
from jax import lax
from jax.experimental import pallas as pl
from jax.experimental.pallas import tpu as pltpu
from jax.sharding import PartitionSpec as P

GROUPS = 32
RESNETS = 3
EPS = 1e-06
LANES = 128
MESH = pl.DeviceIdType.MESH
F32 = jnp.float32
BF16 = jnp.bfloat16


def iota(shape, dim):
    return lax.broadcasted_iota(jnp.int32, shape, dim)


def three_parts(values, part):
    high = values.astype(BF16)
    rest = values - high.astype(F32)
    middle = rest.astype(BF16)
    low = (rest - middle.astype(F32)).astype(BF16)
    picked = jnp.where(part == 0, high.astype(F32), jnp.where(part == 1, middle.astype(F32), low.astype(F32)))
    return jnp.where(part < 3, picked, 0.0).astype(BF16)


def gather_matrix(channels):
    shape = (channels, LANES)
    return (iota(shape, 0) // (channels // GROUPS) == iota(shape, 1) % GROUPS).astype(F32).astype(BF16)


def spread_matrix(channels):
    shape = (LANES, channels)
    return (iota(shape, 0) % GROUPS == iota(shape, 1) // (channels // GROUPS)).astype(F32).astype(BF16)


def kernel(
    nblk,
    nrow,
    halves,
    x_hbm,
    gain_in_hbm,
    shift_in_hbm,
    w1_hbm,
    bias_first_hbm,
    sw_hbm,
    short_bias_hbm,
    gains_hbm,
    shifts_hbm,
    wr_hbm,
    biases_hbm,
    outv,
    gain_in,
    shift_in,
    bias_first,
    short_bias,
    gains,
    shifts,
    biases,
    gather1,
    gather2,
    spread1,
    spread2,
    xv,
    w1,
    wr,
    sw,
    v0,
    vs,
    stream,
    a1,
    a2,
    col_s1,
    col_r1,
    row_r1,
    cor_s1,
    cor_r1,
    col_s2,
    col_r2,
    row_r2,
    cor_s2,
    cor_r2,
    stat_s,
    stat_r,
    relay_s,
    relay_r,
    x_sem,
    w_sem,
    p_sem,
    relay_ssem,
    relay_rsem,
    stat_ssem,
    stat_rsem,
    halo_ssem,
    colr_sem,
    rowr_sem,
    corr_sem,
):
    images, height, width, _ = xv.shape
    per = images // halves
    slots = 2 * per
    pixels = height * width
    z = lax.axis_index("blk")
    c = lax.axis_index("rows")
    oc = 1 - c
    right = lax.rem(z + 1, nblk)
    left = lax.rem(z + nblk - 1, nblk)
    me = z * nrow + c
    edge = (height - 1) * (1 - c)
    halo_row = (height + 1) * (1 - c)
    zero_row = (height + 1) * c

    half_way = nblk // 2
    reach = half_way // 2
    far_from = 2 * half_way // 3 + 1

    def at(offset):
        return lax.rem(z + nblk + offset, nblk)

    barrier = pltpu.get_barrier_semaphore()

    def greet(i, carry):
        d = reach - i
        for zz in (at(d), at(-d)):
            for cc in (c, oc):
                pl.semaphore_signal(barrier, 1, device_id={"blk": zz, "rows": cc}, device_id_type=MESH)
        return carry

    lax.fori_loop(0, reach, greet, 0)
    pl.semaphore_signal(barrier, 1, device_id={"rows": oc}, device_id_type=MESH)

    x_copies = [pltpu.make_async_copy(x_hbm.at[i], xv.at[i], x_sem.at[i]) for i in range(images)]
    w_copies = [
        pltpu.make_async_copy(sw_hbm, sw, w_sem.at[0]),
        pltpu.make_async_copy(w1_hbm, w1, w_sem.at[1]),
    ] + [pltpu.make_async_copy(wr_hbm.at[i], wr.at[i], w_sem.at[2 + i]) for i in range(wr_hbm.shape[0])]
    p_copies = [
        pltpu.make_async_copy(source, target, p_sem.at[i])
        for i, (source, target) in enumerate((
            (gain_in_hbm, gain_in), (shift_in_hbm, shift_in), (bias_first_hbm, bias_first), (short_bias_hbm, short_bias),
            (gains_hbm, gains), (shifts_hbm, shifts), (biases_hbm, biases)))
    ]
    for copy in x_copies + p_copies + w_copies:
        copy.start()

    gather1[...] = gather_matrix(gather1.shape[0])
    gather2[...] = gather_matrix(gather2.shape[0])
    spread1[...] = spread_matrix(spread1.shape[1])
    spread2[...] = spread_matrix(spread2.shape[1])
    for a in (a1, a2):
        for i in range(images):
            a[i, zero_row] = jnp.zeros(a.shape[2:], BF16)

    def local_stats(k, h, rows):
        channels = rows[0].shape[1]
        which = iota((16, channels), 0)
        base = jnp.broadcast_to(rows[0], (16, channels))
        for j in range(1, slots):
            base = jnp.where(which % slots == j, rows[j], base)
        lhs = three_parts(base, which // slots)
        dots = jnp.dot(lhs, (gather1 if k == 0 else gather2)[...], preferred_element_type=F32)
        slot_of_row = iota((16, LANES), 0) % slots
        slot_of_lane = iota((16, LANES), 1) // GROUPS
        packed = jnp.sum(jnp.where(slot_of_row == slot_of_lane, dots, 0.0), axis=0, keepdims=True)
        stat_s[k, h] = jnp.broadcast_to(packed, (8, LANES))
        stat_r[k, h, pl.ds(me, 1)] = packed

    def stat_to(k, h, zz, cc):
        pltpu.make_async_remote_copy(
            stat_s.at[k, h, pl.ds(0, 1)], stat_r.at[k, h, pl.ds(me, 1)], stat_ssem.at[k, h], stat_rsem.at[k, h],
            device_id={"blk": zz, "rows": cc}, device_id_type=MESH,
        ).start()

    def send_between(k, hs, high, low):
        def step(i, carry):
            d = high - i
            for zz in (at(d), at(-d)):
                for h in hs:
                    stat_to(k, h, zz, oc)
                    stat_to(k, h, zz, c)
            return carry

        if high >= low:
            lax.fori_loop(0, high - low + 1, step, 0)

    def send_far(k, h):
        stat_to(k, h, at(half_way), oc)
        stat_to(k, h, at(half_way), c)
        send_between(k, (h,), half_way - 1, far_from)

    def send_near(k, h):
        send_between(k, (h,), min(far_from, half_way) - 1, 1)
        stat_to(k, h, z, oc)

    def wait_stats(k, h):
        count = (2 * reach + 1 if k == 0 else nblk) * nrow - 1
        copy = pltpu.make_async_remote_copy(
            stat_r.at[k, h, pl.ds(0, count)], stat_r.at[k, h, pl.ds(0, count)],
            stat_ssem.at[k, h], stat_rsem.at[k, h], device_id={"rows": oc}, device_id_type=MESH,
        )
        copy.wait_send()
        copy.wait_recv()

    def offset_of_row():
        return lax.rem(iota((nblk * nrow, LANES), 0) // nrow + nblk - z, nblk)

    def relay_copies(h, cores):
        copies = []
        for side, zz in enumerate((at(-reach), at(reach))):
            for i, cc in enumerate(cores):
                copies.append(pltpu.make_async_remote_copy(
                    relay_s.at[h, side, pl.ds(0, 1)], relay_r.at[h, side, pl.ds(0, 1)], relay_ssem.at[h, side, i], relay_rsem.at[h, side],
                    device_id={"blk": zz, "rows": cc}, device_id_type=MESH))
        return copies

    def relay():
        offset = offset_of_row()
        for h in range(halves):
            everything = stat_r[0, h]
            for side, (low, high) in enumerate(((1, reach), (nblk - reach + 1, nblk - 1))):
                inside = jnp.logical_and(offset >= low, offset <= high)
                part = jnp.sum(jnp.where(inside, everything, 0.0), axis=0, keepdims=True)
                relay_s[h, side] = jnp.broadcast_to(part, (8, LANES))
        for h in range(halves):
            for copy in relay_copies(h, (oc, c)):
                copy.start()

    def relay_wait(h):
        for copy in relay_copies(h, (oc,)):
            copy.wait_recv()

    def scales(k, h, channels, gain, shift):
        count = pixels * nblk * nrow * (channels // GROUPS)
        everything = stat_r[k, h]
        if k == 0:
            offset = offset_of_row()
            inside = jnp.logical_or(offset <= reach, offset >= nblk - reach)
            everything = jnp.where(inside, everything, 0.0)
        total = jnp.sum(everything, axis=0, keepdims=True)
        if k == 0:
            total = total + relay_r[h, 0, 0:1] + relay_r[h, 1, 0:1]
        row = iota((16, LANES), 0)
        stat = jnp.where(iota((16, LANES), 1) // GROUPS == row % slots, total * (1.0 / count), 0.0)
        lhs = three_parts(stat, row // slots)
        dots = jnp.dot(lhs, (spread1 if k == 0 else spread2)[...], preferred_element_type=F32)
        pick = lambda j: dots[j : j + 1] + dots[slots + j : slots + j + 1] + dots[2 * slots + j : 2 * slots + j + 1]
        result = []
        for i in range(per):
            center = pick(2 * i)
            a = lax.rsqrt(jnp.maximum(pick(2 * i + 1) - center * center, 0.0) + EPS) * gain
            result.append((0.5 * a, 0.5 * (shift - center * a)))
        return result

    def activate(values, ab):
        half = values * ab[0] + ab[1]
        return half + half * jnp.tanh(half)

    class Halo:
        pass

    def halo_of(k):
        o = Halo()
        first = k == 0
        o.v = v0 if first else vs.at[k - 1]
        o.col_s = col_s1 if first else col_s2.at[k - 1]
        o.col_r = col_r1 if first else col_r2.at[k - 1]
        o.row_r = row_r1 if first else row_r2.at[k - 1]
        o.cor_s = cor_s1 if first else cor_s2.at[k - 1]
        o.cor_r = cor_r1 if first else cor_r2.at[k - 1]
        o.channels = o.v.shape[-1]
        return o

    def halo_copies(k, h):
        o = halo_of(k)
        copies = []
        for side, (near, blk) in enumerate(((0, right), (1, left))):
            copies.append(pltpu.make_async_remote_copy(
                o.col_s.at[h, side], o.col_r.at[h, side], halo_ssem.at[k, h, 2 * side], colr_sem.at[k, h, side],
                device_id={"blk": blk, "rows": c}, device_id_type=MESH))
            copies.append(pltpu.make_async_remote_copy(
                o.cor_s.at[h, side], o.cor_r.at[h, side], halo_ssem.at[k, h, 2 * side + 1], corr_sem.at[k, h, side],
                device_id={"blk": blk, "rows": oc}, device_id_type=MESH))
        copies.append(pltpu.make_async_remote_copy(
            o.v.at[pl.ds(h * per, per), pl.ds(edge * width, width)], o.row_r.at[h], halo_ssem.at[k, h, 4], rowr_sem.at[k, h],
            device_id={"rows": oc}, device_id_type=MESH))
        return copies

    def prepare_halo(k, h):
        o = halo_of(k)
        for side in range(2):
            q = width - 1 if side == 0 else 0
            cols = []
            corners = []
            for i in range(per):
                image = h * per + i
                which = iota((height, o.channels), 0)
                col = jnp.broadcast_to(o.v[image, pl.ds(q, 1), :], (height, o.channels))
                for r in range(1, height):
                    col = jnp.where(which == r, o.v[image, pl.ds(r * width + q, 1), :], col)
                cols.append(col)
                corners.append(o.v[image, pl.ds(edge * width + q, 1), :])
            o.col_s[h, side] = jnp.concatenate(cols, axis=0).astype(BF16)
            for i in range(per):
                o.cor_s[h, side, pl.ds(i, 1)] = corners[i]

    def finish_sends(k, h):
        send_near(k, h)
        for copy in halo_copies(k, h):
            copy.start()

    def await_all(k, h):
        if k == 0:
            relay_wait(h)
        else:
            wait_stats(k, h)
        for copy in halo_copies(k, h):
            copy.wait()

    def load(k, h, a, gain, shift):
        o = halo_of(k)
        channels = o.channels
        factors = scales(k, h, channels, gain, shift)
        column = iota((width, channels), 0)

        def put(image, row, act, low, high):
            a[image, row, :, pl.ds(0, channels)] = jnp.where(column == 0, low, pltpu.roll(act, 1, 0)).astype(BF16)
            a[image, row, :, pl.ds(channels, channels)] = act.astype(BF16)
            a[image, row, :, pl.ds(2 * channels, channels)] = jnp.where(
                column == width - 1, high, pltpu.roll(act, width - 1, 0)).astype(BF16)

        for i in range(per):
            image = h * per + i
            ab = factors[i]
            sides = [activate(o.col_r[h, s, pl.ds(i * height, height)].astype(F32), ab) for s in range(2)]
            corner = [activate(o.cor_r[h, s, pl.ds(i, 1)], ab) for s in range(2)]
            for r in range(height):
                act = activate(o.v[image, pl.ds(r * width, width), :], ab)
                put(image, r + 1, act, sides[0][r : r + 1], sides[1][r : r + 1])
            act = activate(o.row_r[h, i], ab)
            put(image, halo_row, act, corner[0], corner[1])

    def convolve(a, image, weight):
        depth = a.shape[-1]
        total = None
        for d in range(3):
            lhs = a[image, d : d + height].reshape(pixels, depth)
            term = jnp.dot(lhs, weight[d].reshape(depth, weight.shape[-1]), preferred_element_type=F32)
            total = term if total is None else total + term
        return total

    def sums(values):
        return [jnp.sum(values, axis=0, keepdims=True), jnp.sum(values * values, axis=0, keepdims=True)]

    for copy in x_copies:
        copy.wait()
    rows0 = []
    for image in range(images):
        values = xv[image].reshape(pixels, xv.shape[-1]).astype(F32)
        v0[image] = values
        rows0.append(sums(values))
    for h in range(halves):
        local_stats(0, h, sum(rows0[h * per : (h + 1) * per], []))
        prepare_halo(0, h)
    pl.semaphore_wait(barrier, (2 * reach + 1) * nrow - 1)
    send_between(0, range(halves), reach, 1)
    for h in range(halves):
        stat_to(0, h, z, oc)
        for copy in halo_copies(0, h):
            copy.start()

    for copy in p_copies:
        copy.wait()
    w_copies[0].wait()
    for image in range(images):
        stream[image] = jnp.dot(
            xv[image].reshape(pixels, xv.shape[-1]), sw[...], preferred_element_type=F32) + short_bias[...]

    for h in range(halves):
        wait_stats(0, h)

    @pl.when(c == nrow - 1)
    def _():
        relay()

    last = 2 * RESNETS - 1
    for k in range(2 * RESNETS):
        if k == 0:
            a, gain, shift, weight, bias = a1, gain_in, shift_in, w1, bias_first
        else:
            j = pl.ds(k - 1, 1)
            a, gain, shift, weight, bias = a2, gains.at[j], shifts.at[j], wr.at[k - 1], biases.at[j]
        w_copies[1 + k].wait()
        for h in range(halves):
            await_all(k, h)
            load(k, h, a, gain[...], shift[...])
            rows = []
            for i in range(per):
                image = h * per + i
                result = convolve(a, image, weight) + bias[...]
                if k % 2 == 1:
                    result = result + stream[image]
                rounded = result.astype(BF16)
                if k == last:
                    outv[image] = rounded.reshape(height, width, rounded.shape[-1])
                else:
                    values = rounded.astype(F32)
                    vs[k, image] = values
                    if k % 2 == 1:
                        stream[image] = values
                    rows += sums(values)
            if k < last:
                local_stats(k + 1, h, rows)
                send_far(k + 1, h)
                prepare_halo(k + 1, h)
        if k < last:
            for h in range(halves):
                finish_sends(k + 1, h)

    @pl.when(c == nrow - 1)
    def _():
        for h in range(halves):
            for copy in relay_copies(h, (oc, c)):
                copy.wait_send()


def run(nblk, nrow, halves, *args):
    x = args[0]
    w1, wr = args[3], args[9]
    images, height, width, cin = x.shape
    ch = w1.shape[-1]
    per = images // halves
    stages = 2 * RESNETS
    anywhere = pl.BlockSpec(memory_space=pl.ANY)
    inside = pl.BlockSpec(memory_space=pltpu.VMEM)
    specs = [anywhere] * len(args)
    fixed = list(args)
    for j in (1, 2, 4, 6):
        fixed[j] = args[j].reshape(1, -1)

    def halo_buffers(lead, channels):
        return [
            pltpu.VMEM((*lead, halves, 2, per * height, channels), BF16),
            pltpu.VMEM((*lead, halves, 2, per * height, channels), BF16),
            pltpu.VMEM((*lead, halves, per, width, channels), F32),
            pltpu.VMEM((*lead, halves, 2, 8, channels), F32),
            pltpu.VMEM((*lead, halves, 2, 8, channels), F32),
        ]

    return pl.pallas_call(
        functools.partial(kernel, nblk, nrow, halves),
        out_shape=pltpu.VMEM((images, height, width, ch), BF16),
        in_specs=specs,
        out_specs=inside,
        scratch_shapes=[
            *[pltpu.VMEM(fixed[j].shape, F32) for j in (1, 2, 4, 6, 7, 8, 10)],
            pltpu.VMEM((cin, LANES), BF16),
            pltpu.VMEM((ch, LANES), BF16),
            pltpu.VMEM((LANES, cin), BF16),
            pltpu.VMEM((LANES, ch), BF16),
            pltpu.VMEM(x.shape, BF16),
            pltpu.VMEM(w1.shape, BF16),
            pltpu.VMEM(wr.shape, BF16),
            pltpu.VMEM((cin, ch), BF16),
            pltpu.VMEM((images, height * width, cin), F32),
            pltpu.VMEM((stages - 1, images, height * width, ch), F32),
            pltpu.VMEM((images, height * width, ch), F32),
            pltpu.VMEM((images, height + 2, width, 3 * cin), BF16),
            pltpu.VMEM((images, height + 2, width, 3 * ch), BF16),
            *halo_buffers((), cin),
            *halo_buffers((stages - 1,), ch),
            pltpu.VMEM((stages, halves, 8, LANES), F32),
            pltpu.VMEM((stages, halves, nblk * nrow, LANES), F32),
            pltpu.VMEM((halves, 2, 8, LANES), F32),
            pltpu.VMEM((halves, 2, 8, LANES), F32),
            pltpu.SemaphoreType.DMA((images,)),
            pltpu.SemaphoreType.DMA((1 + stages,)),
            pltpu.SemaphoreType.DMA((7,)),
            pltpu.SemaphoreType.DMA((halves, 2, 2)),
            pltpu.SemaphoreType.DMA((halves, 2)),
            pltpu.SemaphoreType.DMA((stages, halves)),
            pltpu.SemaphoreType.DMA((stages, halves)),
            pltpu.SemaphoreType.DMA((stages, halves, 5)),
            pltpu.SemaphoreType.DMA((stages, halves, 2)),
            pltpu.SemaphoreType.DMA((stages, halves)),
            pltpu.SemaphoreType.DMA((stages, halves, 2)),
        ],
        compiler_params=pltpu.CompilerParams(
            collective_id=0, has_side_effects=True, vmem_limit_bytes=60 * 1024 * 1024),
    )(*fixed)


def solution(mesh):
    placed = (P("groups", "rows", "blk", None),) + (P(),) * 10
    return jax.shard_map(
        functools.partial(run, mesh.shape["blk"], mesh.shape["rows"], 2),
        mesh=mesh,
        in_specs=placed,
        out_specs=P("groups", "rows", "blk", None),
        check_vma=False,
    )
```

```python
import functools

import jax
import jax.numpy as jnp
from jax import lax
from jax.experimental import pallas as pl
from jax.experimental.pallas import tpu as pltpu
from jax.sharding import PartitionSpec as P

GROUPS = 32
RESNETS = 3
EPS = 1e-06
LANES = 128
TAPS = (1, 0, 2)
MESH = pl.DeviceIdType.MESH
F32 = jnp.float32
BF16 = jnp.bfloat16


def iota(shape, dim):
    return lax.broadcasted_iota(jnp.int32, shape, dim)


def three_parts(values, part):
    high = values.astype(BF16)
    rest = values - high.astype(F32)
    middle = rest.astype(BF16)
    low = (rest - middle.astype(F32)).astype(BF16)
    picked = jnp.where(part == 0, high.astype(F32), jnp.where(part == 1, middle.astype(F32), low.astype(F32)))
    return jnp.where(part < 3, picked, 0.0).astype(BF16)


def gather_matrix(channels):
    shape = (channels, LANES)
    return (iota(shape, 0) // (channels // GROUPS) == iota(shape, 1) % GROUPS).astype(F32).astype(BF16)


def spread_matrix(channels):
    shape = (LANES, channels)
    return (iota(shape, 0) % GROUPS == iota(shape, 1) // (channels // GROUPS)).astype(F32).astype(BF16)


def kernel(
    nblk,
    nrow,
    halves,
    x_hbm,
    gain_in_hbm,
    shift_in_hbm,
    w1_hbm,
    bias_first_hbm,
    sw_hbm,
    short_bias_hbm,
    gains_hbm,
    shifts_hbm,
    wr_hbm,
    biases_hbm,
    outv,
    gain_in,
    shift_in,
    bias_first,
    short_bias,
    gains,
    shifts,
    biases,
    gather1,
    gather2,
    spread1,
    spread2,
    xv,
    w1,
    wr,
    sw,
    v0,
    vs,
    short,
    s1,
    s2,
    a1,
    a2,
    col_s1,
    col_r1,
    row_r1,
    cor_s1,
    cor_r1,
    col_s2,
    col_r2,
    row_r2,
    cor_s2,
    cor_r2,
    stat_s,
    stat_r,
    relay_s,
    relay_r,
    x_sem,
    w_sem,
    p_sem,
    relay_ssem,
    relay_rsem,
    stat_ssem,
    stat_rsem,
    halo_ssem,
    colr_sem,
    rowr_sem,
    corr_sem,
):
    images, height, width, _ = xv.shape
    per = images // halves
    slots = 2 * per
    pixels = height * width
    z = lax.axis_index("blk")
    c = lax.axis_index("rows")
    oc = 1 - c
    right = lax.rem(z + 1, nblk)
    left = lax.rem(z + nblk - 1, nblk)
    me = z * nrow + c
    edge = height - 1

    def mirrored(row, rows):
        return row + c * (rows - 1 - 2 * row)


    half_way = nblk // 2
    reach = -(-half_way // 3)
    leap = half_way - reach
    far_from = 2 * half_way // 3 + 1

    def at(offset):
        return lax.rem(z + nblk + offset, nblk)

    barrier = pltpu.get_barrier_semaphore()

    def greet(i, carry):
        d = reach - i
        for zz in (at(d), at(-d)):
            for cc in (c, oc):
                pl.semaphore_signal(barrier, 1, device_id={"blk": zz, "rows": cc}, device_id_type=MESH)
        return carry

    lax.fori_loop(0, reach, greet, 0)
    pl.semaphore_signal(barrier, 1, device_id={"rows": oc}, device_id_type=MESH)

    x_waits = [pltpu.make_async_copy(x_hbm.at[i], xv.at[i], x_sem.at[i]) for i in range(images)]
    x_copies = [
        pltpu.make_async_copy(x_hbm.at[i, mirrored(r, height)], xv.at[i, r], x_sem.at[i])
        for i in range(images) for r in range(height)
    ]
    kernels = [(w1_hbm, w1)] + [(wr_hbm.at[i], wr.at[i]) for i in range(wr_hbm.shape[0])]
    w_waits = [pltpu.make_async_copy(sw_hbm, sw, w_sem.at[0])]
    w_copies = [w_waits[0]]
    for i, (source, target) in enumerate(kernels):
        w_waits.append(pltpu.make_async_copy(source, target, w_sem.at[1 + i]))
        for slot, tap in enumerate(TAPS):
            for d in range(3):
                w_copies.append(pltpu.make_async_copy(source.at[mirrored(d, 3), tap], target.at[d, slot], w_sem.at[1 + i]))
    p_copies = [
        pltpu.make_async_copy(source, target, p_sem.at[i])
        for i, (source, target) in enumerate((
            (gain_in_hbm, gain_in), (shift_in_hbm, shift_in), (bias_first_hbm, bias_first), (short_bias_hbm, short_bias),
            (gains_hbm, gains), (shifts_hbm, shifts), (biases_hbm, biases)))
    ]
    for copy in x_copies + p_copies + w_copies:
        copy.start()

    gather1[...] = gather_matrix(gather1.shape[0])
    gather2[...] = gather_matrix(gather2.shape[0])
    spread1[...] = spread_matrix(spread1.shape[1])
    spread2[...] = spread_matrix(spread2.shape[1])
    for a in (a1, a2):
        for i in range(images):
            a[i, 0] = jnp.zeros(a.shape[2:], BF16)

    def local_stats(k, h, rows):
        channels = rows[0].shape[1]
        which = iota((16, channels), 0)
        base = jnp.broadcast_to(rows[0], (16, channels))
        for j in range(1, slots):
            base = jnp.where(which % slots == j, rows[j], base)
        lhs = three_parts(base, which // slots)
        dots = jnp.dot(lhs, (gather1 if k == 0 else gather2)[...], preferred_element_type=F32)
        slot_of_row = iota((16, LANES), 0) % slots
        slot_of_lane = iota((16, LANES), 1) // GROUPS
        packed = jnp.sum(jnp.where(slot_of_row == slot_of_lane, dots, 0.0), axis=0, keepdims=True)
        stat_s[k, h] = jnp.broadcast_to(packed, (8, LANES))

    def stat_to(k, h, zz, cc):
        pltpu.make_async_remote_copy(
            stat_s.at[k, h, pl.ds(0, 1)], stat_r.at[k, h, pl.ds(me, 1)], stat_ssem.at[k, h], stat_rsem.at[k, h],
            device_id={"blk": zz, "rows": cc}, device_id_type=MESH,
        ).start()

    def send_between(k, hs, high, low):
        def step(i, carry):
            d = high - i
            for zz in (at(d), at(-d)):
                for h in hs:
                    stat_to(k, h, zz, oc)
                    stat_to(k, h, zz, c)
            return carry

        if high >= low:
            lax.fori_loop(0, high - low + 1, step, 0)

    def send_far(k, h):
        stat_to(k, h, at(half_way), oc)
        stat_to(k, h, at(half_way), c)
        send_between(k, (h,), half_way - 1, far_from)

    def send_near(k, h):
        send_between(k, (h,), far_from - 1, 1)
        stat_to(k, h, z, oc)

    def wait_stats(k, h):
        count = (2 * reach + 1 if k == 0 else nblk) * nrow - 1
        copy = pltpu.make_async_remote_copy(
            stat_r.at[k, h, pl.ds(0, count)], stat_r.at[k, h, pl.ds(0, count)],
            stat_ssem.at[k, h], stat_rsem.at[k, h], device_id={"rows": oc}, device_id_type=MESH,
        )
        copy.wait_send()
        copy.wait_recv()

    def gathered(k, h):
        own = iota((nblk * nrow, LANES), 0) == me
        return jnp.where(own, stat_s[k, h, 0:1], stat_r[k, h])

    def between(low, high):
        chip = iota((nblk * nrow, LANES), 0) // nrow
        return lax.rem(chip + 2 * nblk - z - low, nblk) <= high - low

    def relay_copies(h, cores):
        copies = []
        for side, zz in enumerate((at(-leap), at(leap))):
            for i, cc in enumerate(cores):
                copies.append(pltpu.make_async_remote_copy(
                    relay_s.at[h, side, pl.ds(0, 1)], relay_r.at[h, side, pl.ds(0, 1)], relay_ssem.at[h, side, i], relay_rsem.at[h, side],
                    device_id={"blk": zz, "rows": cc}, device_id_type=MESH))
        return copies

    def relay():
        for h in range(halves):
            everything = gathered(0, h)
            for side, (low, high) in enumerate(((reach + 1 - leap, reach), (1 - reach, leap - reach - 1))):
                part = jnp.sum(jnp.where(between(low, high), everything, 0.0), axis=0, keepdims=True)
                relay_s[h, side] = jnp.broadcast_to(part, (8, LANES))
        for h in range(halves):
            for copy in relay_copies(h, (oc, c)):
                copy.start()

    def relay_wait(h):
        for copy in relay_copies(h, (oc,)):
            copy.wait_recv()

    def scales(k, h, channels, gain, shift):
        count = pixels * nblk * nrow * (channels // GROUPS)
        everything = gathered(k, h)
        if k == 0:
            everything = jnp.where(between(-reach, reach), everything, 0.0)
        total = jnp.sum(everything, axis=0, keepdims=True)
        if k == 0:
            total = total + relay_r[h, 0, 0:1] + relay_r[h, 1, 0:1]
        row = iota((16, LANES), 0)
        stat = jnp.where(iota((16, LANES), 1) // GROUPS == row % slots, total * (1.0 / count), 0.0)
        lhs = three_parts(stat, row // slots)
        dots = jnp.dot(lhs, (spread1 if k == 0 else spread2)[...], preferred_element_type=F32)
        pick = lambda j: dots[j : j + 1] + dots[slots + j : slots + j + 1] + dots[2 * slots + j : 2 * slots + j + 1]
        result = []
        for i in range(per):
            center = pick(2 * i)
            a = lax.rsqrt(jnp.maximum(pick(2 * i + 1) - center * center, 0.0) + EPS) * gain
            result.append((0.5 * a, 0.5 * (shift - center * a)))
        return result

    def activate(values, ab):
        half = values * ab[0] + ab[1]
        return half + half * jnp.tanh(half)

    class Halo:
        pass

    def halo_of(k):
        o = Halo()
        first = k == 0
        o.v = v0 if first else vs.at[k - 1]
        o.col_s = col_s1 if first else col_s2.at[k - 1]
        o.col_r = col_r1 if first else col_r2.at[k - 1]
        o.row_r = row_r1 if first else row_r2.at[k - 1]
        o.cor_s = cor_s1 if first else cor_s2.at[k - 1]
        o.cor_r = cor_r1 if first else cor_r2.at[k - 1]
        o.tiles = o.v.shape[1]
        o.channels = o.tiles * LANES
        return o

    def halo_copies(k, h):
        o = halo_of(k)
        copies = []
        for side, (near, blk) in enumerate(((0, right), (1, left))):
            copies.append(pltpu.make_async_remote_copy(
                o.col_s.at[h, side], o.col_r.at[h, side], halo_ssem.at[k, h, 2 * side], colr_sem.at[k, h, side],
                device_id={"blk": blk, "rows": c}, device_id_type=MESH))
            copies.append(pltpu.make_async_remote_copy(
                o.cor_s.at[h, side, pl.ds(0, per)], o.cor_r.at[h, side, pl.ds(0, per)], halo_ssem.at[k, h, 2 * side + 1], corr_sem.at[k, h, side],
                device_id={"blk": blk, "rows": oc}, device_id_type=MESH))
        copies.append(pltpu.make_async_remote_copy(
            o.v.at[pl.ds(h * per, per), :, pl.ds(edge * width, width)], o.row_r.at[h], halo_ssem.at[k, h, 4], rowr_sem.at[k, h],
            device_id={"rows": oc}, device_id_type=MESH))
        return copies

    def prepare_halo(k, h):
        o = halo_of(k)
        for side in range(2):
            q = width - 1 if side == 0 else 0
            for t in range(o.tiles):
                lanes = pl.ds(t * LANES, LANES)
                cols = [o.v[h * per + i, t, pl.ds(q, height, stride=width), :] for i in range(per)]
                o.col_s[h, side, :, lanes] = jnp.concatenate(cols, axis=0).astype(BF16)
                for i in range(per):
                    o.cor_s[h, side, pl.ds(i, 1), lanes] = o.v[h * per + i, t, pl.ds(edge * width + q, 1), :]

    def finish_sends(k, h):
        send_near(k, h)
        for copy in halo_copies(k, h):
            copy.start()

    def await_all(k, h):
        for copy in halo_copies(k, h):
            copy.wait()
        if k == 0:
            relay_wait(h)
        else:
            wait_stats(k, h)

    def load(k, h, a, gain, shift):
        o = halo_of(k)
        channels = o.channels
        factors = scales(k, h, channels, gain, shift)
        pitch = width + 16
        for i in range(per):
            image = h * per + i
            shelf = s1.at[image] if k == 0 else s2.at[i]
            tiles = [slice(t * LANES, (t + 1) * LANES) for t in range(o.tiles)]
            ab = [[x[:, t] for x in factors[i]] for t in tiles]

            for s, at_column in enumerate((7, width + 8)):
                for t, lanes in enumerate(tiles):
                    side = activate(o.col_r[h, s, pl.ds(i * height, height), lanes].astype(F32), ab[t])
                    shelf[t, pl.ds(at_column, height, stride=pitch), :] = side
                    shelf[t, pl.ds(height * pitch + at_column, 1), :] = activate(o.cor_r[h, s, pl.ds(i, 1), lanes], ab[t])
            for r in range(height + 1):
                center = []
                for t in range(o.tiles):
                    source = o.v[image, t, pl.ds(r * width, width), :] if r < height else o.row_r[h, i, t]
                    act = activate(source, ab[t])
                    shelf[t, pl.ds(r * pitch + 8, width), :] = act
                    center.append(act)
                a[image, r + 1, :, pl.ds(0, channels)] = jnp.concatenate(center, axis=1).astype(BF16)
            for slot in (1, 2):
                for r in range(height + 1):
                    moved = [shelf[t, pl.ds(r * pitch + 7 + TAPS[slot], width), :] for t in range(o.tiles)]
                    a[image, r + 1, :, pl.ds(slot * channels, channels)] = jnp.concatenate(moved, axis=1).astype(BF16)

    def convolve(a, image, weight):
        depth = a.shape[-1]
        total = None
        step = depth // 3
        for slot in range(3):
            for d in TAPS:
                lhs = a[image, d : d + height, :, pl.ds(slot * step, step)].reshape(pixels, step)
                term = jnp.dot(lhs, weight[d, slot], preferred_element_type=F32)
                total = term if total is None else total + term
        return total

    def put(target, values):
        for t in range(target.shape[0]):
            target[t] = values[:, t * LANES : (t + 1) * LANES]

    def sums(values):
        return [jnp.sum(values, axis=0, keepdims=True), jnp.sum(values * values, axis=0, keepdims=True)]

    for copy in x_waits:
        copy.wait()
    rows0 = []
    for image in range(images):
        values = xv[image].reshape(pixels, xv.shape[-1]).astype(F32)
        put(v0.at[image], values)
        rows0.append(sums(values))
    for h in range(halves):
        local_stats(0, h, sum(rows0[h * per : (h + 1) * per], []))
        prepare_halo(0, h)
    pl.semaphore_wait(barrier, (2 * reach + 1) * nrow - 1)
    send_between(0, range(halves), reach, 1)
    for h in range(halves):
        stat_to(0, h, z, oc)
        for copy in halo_copies(0, h):
            copy.start()

    for copy in p_copies:
        copy.wait()
    w_waits[0].wait()
    for image in range(images):
        put(short.at[image], jnp.dot(
            xv[image].reshape(pixels, xv.shape[-1]), sw[...], preferred_element_type=F32) + short_bias[...])

    for h in range(halves):
        wait_stats(0, h)

    @pl.when(c == nrow - 1)
    def _():
        relay()

    last = 2 * RESNETS - 1
    for k in range(2 * RESNETS):
        if k == 0:
            a, gain, shift, weight, bias = a1, gain_in, shift_in, w1, bias_first
        else:
            j = pl.ds(k - 1, 1)
            a, gain, shift, weight, bias = a2, gains.at[j], shifts.at[j], wr.at[k - 1], biases.at[j]
        w_waits[1 + k].wait()
        for h in range(halves):
            if k > 0:
                await_all(k, h)
                load(k, h, a, gain[...], shift[...])
            elif h == 0:
                for g in range(halves):
                    await_all(k, g)
                for g in range(halves):
                    load(k, g, a, gain[...], shift[...])
            rows = []
            for i in range(per):
                image = h * per + i
                result = convolve(a, image, weight) + bias[...]
                if k % 2 == 1:
                    skip = short.at[image] if k == 1 else vs.at[k - 2, image]
                    result = result + jnp.concatenate([skip[t] for t in range(skip.shape[0])], axis=1)
                rounded = result.astype(BF16)
                if k == last:
                    for r in range(height):
                        outv[image, mirrored(r, height)] = rounded[r * width : (r + 1) * width]
                else:
                    values = rounded.astype(F32)
                    put(vs.at[k, image], values)
                    rows += sums(values)
            if k < last:
                local_stats(k + 1, h, rows)
                send_far(k + 1, h)
                prepare_halo(k + 1, h)
        if k < last:
            for h in range(halves):
                finish_sends(k + 1, h)

    @pl.when(c == nrow - 1)
    def _():
        for h in range(halves):
            for copy in relay_copies(h, (oc, c)):
                copy.wait_send()


def run(nblk, nrow, halves, *args):
    x = args[0]
    w1, wr = args[3], args[9]
    images, height, width, cin = x.shape
    ch = w1.shape[-1]
    per = images // halves
    stages = 2 * RESNETS
    anywhere = pl.BlockSpec(memory_space=pl.ANY)
    inside = pl.BlockSpec(memory_space=pltpu.VMEM)
    specs = [anywhere] * len(args)
    fixed = list(args)
    for j in (1, 2, 4, 6):
        fixed[j] = args[j].reshape(1, -1)

    def halo_buffers(lead, channels):
        return [
            pltpu.VMEM((*lead, halves, 2, per * height, channels), BF16),
            pltpu.VMEM((*lead, halves, 2, per * height, channels), BF16),
            pltpu.VMEM((*lead, halves, per, channels // LANES, width, LANES), F32),
            pltpu.VMEM((*lead, halves, 2, 8, channels), F32),
            pltpu.VMEM((*lead, halves, 2, 8, channels), F32),
        ]

    return pl.pallas_call(
        functools.partial(kernel, nblk, nrow, halves),
        out_shape=pltpu.VMEM((images, height, width, ch), BF16),
        in_specs=specs,
        out_specs=inside,
        scratch_shapes=[
            *[pltpu.VMEM(fixed[j].shape, F32) for j in (1, 2, 4, 6, 7, 8, 10)],
            pltpu.VMEM((cin, LANES), BF16),
            pltpu.VMEM((ch, LANES), BF16),
            pltpu.VMEM((LANES, cin), BF16),
            pltpu.VMEM((LANES, ch), BF16),
            pltpu.VMEM(x.shape, BF16),
            pltpu.VMEM(w1.shape, BF16),
            pltpu.VMEM(wr.shape, BF16),
            pltpu.VMEM((cin, ch), BF16),
            pltpu.VMEM((images, cin // LANES, height * width, LANES), F32),
            pltpu.VMEM((stages - 1, images, ch // LANES, height * width, LANES), F32),
            pltpu.VMEM((images, ch // LANES, height * width, LANES), F32),
            pltpu.VMEM((images, cin // LANES, (height + 1) * (width + 16), LANES), F32),
            pltpu.VMEM((per, ch // LANES, (height + 1) * (width + 16), LANES), F32),
            pltpu.VMEM((images, height + 2, width, 3 * cin), BF16),
            pltpu.VMEM((images, height + 2, width, 3 * ch), BF16),
            *halo_buffers((), cin),
            *halo_buffers((stages - 1,), ch),
            pltpu.VMEM((stages, halves, 8, LANES), F32),
            pltpu.VMEM((stages, halves, nblk * nrow, LANES), F32),
            pltpu.VMEM((halves, 2, 8, LANES), F32),
            pltpu.VMEM((halves, 2, 8, LANES), F32),
            pltpu.SemaphoreType.DMA((images,)),
            pltpu.SemaphoreType.DMA((1 + stages,)),
            pltpu.SemaphoreType.DMA((7,)),
            pltpu.SemaphoreType.DMA((halves, 2, 2)),
            pltpu.SemaphoreType.DMA((halves, 2)),
            pltpu.SemaphoreType.DMA((stages, halves)),
            pltpu.SemaphoreType.DMA((stages, halves)),
            pltpu.SemaphoreType.DMA((stages, halves, 5)),
            pltpu.SemaphoreType.DMA((stages, halves, 2)),
            pltpu.SemaphoreType.DMA((stages, halves)),
            pltpu.SemaphoreType.DMA((stages, halves, 2)),
        ],
        compiler_params=pltpu.CompilerParams(
            collective_id=0, has_side_effects=True, vmem_limit_bytes=60 * 1024 * 1024),
    )(*fixed)


def solution(mesh):
    placed = (P("groups", "rows", "blk", None),) + (P(),) * 10
    return jax.shard_map(
        functools.partial(run, mesh.shape["blk"], mesh.shape["rows"], 2),
        mesh=mesh,
        in_specs=placed,
        out_specs=P("groups", "rows", "blk", None),
        check_vma=False,
    )
```

```python
import functools

import jax
import jax.numpy as jnp
from jax import lax
from jax.experimental import pallas as pl
from jax.experimental.pallas import tpu as pltpu
from jax.sharding import PartitionSpec as P

GROUPS = 32
RESNETS = 3
EPS = 1e-06
LANES = 128
TAPS = (1, 0, 2)
MESH = pl.DeviceIdType.MESH
F32 = jnp.float32
BF16 = jnp.bfloat16


def iota(shape, dim):
    return lax.broadcasted_iota(jnp.int32, shape, dim)


def three_parts(values, part):
    high = values.astype(BF16)
    rest = values - high.astype(F32)
    middle = rest.astype(BF16)
    low = (rest - middle.astype(F32)).astype(BF16)
    picked = jnp.where(part == 0, high.astype(F32), jnp.where(part == 1, middle.astype(F32), low.astype(F32)))
    return jnp.where(part < 3, picked, 0.0).astype(BF16)


def gather_matrix(channels):
    shape = (channels, LANES)
    return (iota(shape, 0) // (channels // GROUPS) == iota(shape, 1) % GROUPS).astype(F32).astype(BF16)


def spread_matrix(channels):
    shape = (LANES, channels)
    return (iota(shape, 0) % GROUPS == iota(shape, 1) // (channels // GROUPS)).astype(F32).astype(BF16)


def kernel(
    nblk,
    nrow,
    halves,
    x_hbm,
    gain_in_hbm,
    shift_in_hbm,
    w1_hbm,
    bias_first_hbm,
    sw_hbm,
    short_bias_hbm,
    gains_hbm,
    shifts_hbm,
    wr_hbm,
    biases_hbm,
    outv,
    gain_in,
    shift_in,
    bias_first,
    short_bias,
    gains,
    shifts,
    biases,
    gather1,
    gather2,
    spread1,
    spread2,
    xv,
    w1,
    wr,
    sw,
    v0,
    vs,
    short,
    s1,
    s2,
    a1,
    a2,
    col_s1,
    col_r1,
    row_r1,
    cor_s1,
    cor_r1,
    col_s2,
    col_r2,
    row_r2,
    cor_s2,
    cor_r2,
    stat_s,
    stat_r,
    relay_s,
    relay_r,
    x_sem,
    w_sem,
    p_sem,
    relay_ssem,
    relay_rsem,
    stat_ssem,
    stat_rsem,
    halo_ssem,
    colr_sem,
    rowr_sem,
    corr_sem,
):
    images, height, width, _ = xv.shape
    per = images // halves
    slots = 2 * per
    pixels = height * width
    z = lax.axis_index("blk")
    c = lax.axis_index("rows")
    oc = 1 - c
    right = lax.rem(z + 1, nblk)
    left = lax.rem(z + nblk - 1, nblk)
    me = z * nrow + c
    edge = height - 1

    def mirrored(row, rows):
        return row + c * (rows - 1 - 2 * row)


    half_way = nblk // 2
    reach = -(-half_way // 3)
    leap = half_way - reach

    def at(offset):
        return lax.rem(z + nblk + offset, nblk)

    barrier = pltpu.get_barrier_semaphore()

    def greet(i, carry):
        d = reach - i
        for zz in (at(d), at(-d)):
            for cc in (c, oc):
                pl.semaphore_signal(barrier, 1, device_id={"blk": zz, "rows": cc}, device_id_type=MESH)
        return carry

    lax.fori_loop(0, reach, greet, 0)
    pl.semaphore_signal(barrier, 1, device_id={"rows": oc}, device_id_type=MESH)

    x_waits = [pltpu.make_async_copy(x_hbm.at[i], xv.at[i], x_sem.at[i]) for i in range(images)]
    x_copies = [
        pltpu.make_async_copy(x_hbm.at[i, mirrored(r, height)], xv.at[i, r], x_sem.at[i])
        for i in range(images) for r in range(height)
    ]
    kernels = [(w1_hbm, w1)] + [(wr_hbm.at[i], wr.at[i]) for i in range(wr_hbm.shape[0])]
    w_waits = [pltpu.make_async_copy(sw_hbm, sw, w_sem.at[0])]
    w_copies = [w_waits[0]]
    for i, (source, target) in enumerate(kernels):
        w_waits.append(pltpu.make_async_copy(source, target, w_sem.at[1 + i]))
        for slot, tap in enumerate(TAPS):
            for d in range(3):
                w_copies.append(pltpu.make_async_copy(source.at[mirrored(d, 3), tap], target.at[d, slot], w_sem.at[1 + i]))
    p_copies = [
        pltpu.make_async_copy(source, target, p_sem.at[i])
        for i, (source, target) in enumerate((
            (gain_in_hbm, gain_in), (shift_in_hbm, shift_in), (bias_first_hbm, bias_first), (short_bias_hbm, short_bias),
            (gains_hbm, gains), (shifts_hbm, shifts), (biases_hbm, biases)))
    ]
    for copy in x_copies:
        copy.start()

    gather1[...] = gather_matrix(gather1.shape[0])
    gather2[...] = gather_matrix(gather2.shape[0])
    spread1[...] = spread_matrix(spread1.shape[1])
    spread2[...] = spread_matrix(spread2.shape[1])
    for a in (a1, a2):
        for i in range(images):
            a[i, 0] = jnp.zeros(a.shape[2:], BF16)

    def local_stats(k, h, rows):
        channels = rows[0].shape[1]
        which = iota((16, channels), 0)
        base = jnp.broadcast_to(rows[0], (16, channels))
        for j in range(1, slots):
            base = jnp.where(which % slots == j, rows[j], base)
        lhs = three_parts(base, which // slots)
        dots = jnp.dot(lhs, (gather1 if k == 0 else gather2)[...], preferred_element_type=F32)
        slot_of_row = iota((16, LANES), 0) % slots
        slot_of_lane = iota((16, LANES), 1) // GROUPS
        packed = jnp.sum(jnp.where(slot_of_row == slot_of_lane, dots, 0.0), axis=0, keepdims=True)
        stat_s[k, h] = jnp.broadcast_to(packed, (8, LANES))

    def stat_to(k, h, zz, cc):
        pltpu.make_async_remote_copy(
            stat_s.at[k, h, pl.ds(0, 1)], stat_r.at[k, h, pl.ds(me, 1)], stat_ssem.at[k, h], stat_rsem.at[k, h],
            device_id={"blk": zz, "rows": cc}, device_id_type=MESH,
        ).start()

    def send_between(k, hs, high, low):
        def step(i, carry):
            d = high - i
            for h in hs:
                for zz in (at(d), at(-d)):
                    for cc in range(nrow):
                        stat_to(k, h, zz, cc)
            return carry

        if high >= low:
            lax.fori_loop(0, high - low + 1, step, 0)

    def far_from(k, h):
        return (3 * half_way // 4 if k == 1 and h == 0 else 2 * half_way // 3) + 1

    def send_far(k, h):
        for cc in range(nrow):
            stat_to(k, h, at(half_way), cc)
        send_between(k, (h,), half_way - 1, far_from(k, h))

    def send_near(k, h):
        send_between(k, (h,), min(far_from(k, h), half_way) - 1, 1)
        stat_to(k, h, z, oc)

    def wait_stats(k, h):
        count = (2 * reach + 1 if k == 0 else nblk) * nrow - 1
        copy = pltpu.make_async_remote_copy(
            stat_r.at[k, h, pl.ds(0, count)], stat_r.at[k, h, pl.ds(0, count)],
            stat_ssem.at[k, h], stat_rsem.at[k, h], device_id={"rows": oc}, device_id_type=MESH,
        )
        copy.wait_send()
        copy.wait_recv()

    def gathered(k, h):
        own = iota((nblk * nrow, LANES), 0) == me
        return jnp.where(own, stat_s[k, h, 0:1], stat_r[k, h])

    def between(low, high):
        chip = iota((nblk * nrow, LANES), 0) // nrow
        return lax.rem(chip + 2 * nblk - z - low, nblk) <= high - low

    def relay_copies(h, cores):
        copies = []
        for side, zz in enumerate((at(-leap), at(leap))):
            for i, cc in enumerate(cores):
                copies.append(pltpu.make_async_remote_copy(
                    relay_s.at[h, side, pl.ds(0, 1)], relay_r.at[h, side, pl.ds(0, 1)], relay_ssem.at[h, side, i], relay_rsem.at[h, side],
                    device_id={"blk": zz, "rows": cc}, device_id_type=MESH))
        return copies

    def relay():
        for h in range(halves):
            everything = gathered(0, h)
            for side, (low, high) in enumerate(((reach + 1 - leap, reach), (1 - reach, leap - reach - 1))):
                part = jnp.sum(jnp.where(between(low, high), everything, 0.0), axis=0, keepdims=True)
                relay_s[h, side] = jnp.broadcast_to(part, (8, LANES))
        for h in range(halves):
            for copy in relay_copies(h, (oc, c)):
                copy.start()

    def relay_wait(h):
        for copy in relay_copies(h, (oc,)):
            copy.wait_recv()

    def scales(k, h, channels, gain, shift):
        count = pixels * nblk * nrow * (channels // GROUPS)
        everything = gathered(k, h)
        if k == 0:
            everything = jnp.where(between(-reach, reach), everything, 0.0)
        total = jnp.sum(everything, axis=0, keepdims=True)
        if k == 0:
            total = total + relay_r[h, 0, 0:1] + relay_r[h, 1, 0:1]
        row = iota((16, LANES), 0)
        stat = jnp.where(iota((16, LANES), 1) // GROUPS == row % slots, total * (1.0 / count), 0.0)
        lhs = three_parts(stat, row // slots)
        dots = jnp.dot(lhs, (spread1 if k == 0 else spread2)[...], preferred_element_type=F32)
        pick = lambda j: dots[j : j + 1] + dots[slots + j : slots + j + 1] + dots[2 * slots + j : 2 * slots + j + 1]
        result = []
        for i in range(per):
            center = pick(2 * i)
            a = lax.rsqrt(jnp.maximum(pick(2 * i + 1) - center * center, 0.0) + EPS) * gain
            result.append((0.5 * a, 0.5 * (shift - center * a)))
        return result

    def activate(values, ab):
        half = values * ab[0] + ab[1]
        return half + half * jnp.tanh(half)

    class Halo:
        pass

    def halo_of(k):
        o = Halo()
        first = k == 0
        o.v = v0 if first else vs.at[k - 1]
        o.col_s = col_s1 if first else col_s2.at[k - 1]
        o.col_r = col_r1 if first else col_r2.at[k - 1]
        o.row_r = row_r1 if first else row_r2.at[k - 1]
        o.cor_s = cor_s1 if first else cor_s2.at[k - 1]
        o.cor_r = cor_r1 if first else cor_r2.at[k - 1]
        o.tiles = o.v.shape[1]
        o.channels = o.tiles * LANES
        return o

    def halo_copies(k, h):
        o = halo_of(k)
        copies = []
        for side, (near, blk) in enumerate(((0, right), (1, left))):
            copies.append(pltpu.make_async_remote_copy(
                o.col_s.at[h, side], o.col_r.at[h, side], halo_ssem.at[k, h, 2 * side], colr_sem.at[k, h, side],
                device_id={"blk": blk, "rows": c}, device_id_type=MESH))
            copies.append(pltpu.make_async_remote_copy(
                o.cor_s.at[h, side, pl.ds(0, per)], o.cor_r.at[h, side, pl.ds(0, per)], halo_ssem.at[k, h, 2 * side + 1], corr_sem.at[k, h, side],
                device_id={"blk": blk, "rows": oc}, device_id_type=MESH))
        copies.append(pltpu.make_async_remote_copy(
            o.v.at[pl.ds(h * per, per), :, pl.ds(edge * width, width)], o.row_r.at[h], halo_ssem.at[k, h, 4], rowr_sem.at[k, h],
            device_id={"rows": oc}, device_id_type=MESH))
        return copies

    def prepare_halo(k, h):
        o = halo_of(k)
        for side in range(2):
            q = width - 1 if side == 0 else 0
            for t in range(o.tiles):
                lanes = pl.ds(t * LANES, LANES)
                cols = [o.v[h * per + i, t, pl.ds(q, height, stride=width), :] for i in range(per)]
                o.col_s[h, side, :, lanes] = jnp.concatenate(cols, axis=0).astype(BF16)
                corner = edge * width + q
                block = jnp.zeros((8, LANES), F32)
                for i in range(per):
                    around = o.v[h * per + i, t, pl.ds(corner // 8 * 8, 8), :]
                    block = jnp.where(iota((8, LANES), 0) == i, around[corner % 8 : corner % 8 + 1], block)
                o.cor_s[h, side, :, lanes] = block

    def finish_sends(k, h):
        send_near(k, h)
        for copy in halo_copies(k, h):
            copy.start()

    def await_all(k, h):
        for copy in halo_copies(k, h):
            copy.wait()
        if k == 0:
            relay_wait(h)
        else:
            wait_stats(k, h)

    def load(k, h, a, gain, shift):
        o = halo_of(k)
        channels = o.channels
        factors = scales(k, h, channels, gain, shift)
        pitch = width + 16
        for i in range(per):
            image = h * per + i
            shelf = (s1 if k == 0 else s2).at[i]
            tiles = [slice(t * LANES, (t + 1) * LANES) for t in range(o.tiles)]
            ab = [[x[:, t] for x in factors[i]] for t in tiles]

            for s, at_column in enumerate((7, width + 8)):
                for t, lanes in enumerate(tiles):
                    side = activate(o.col_r[h, s, pl.ds(i * height, height), lanes].astype(F32), ab[t])
                    shelf[t, pl.ds(at_column, height, stride=pitch), :] = side
                    shelf[t, pl.ds(height * pitch + at_column, 1), :] = activate(o.cor_r[h, s, :, lanes][i : i + 1], ab[t])
            for r in range(height + 1):
                center = []
                for t in range(o.tiles):
                    source = o.v[image, t, pl.ds(r * width, width), :] if r < height else o.row_r[h, i, t]
                    act = activate(source, ab[t])
                    shelf[t, pl.ds(r * pitch + 8, width), :] = act
                    center.append(act)
                a[image, r + 1, :, pl.ds(0, channels)] = jnp.concatenate(center, axis=1).astype(BF16)
            for slot in (1, 2):
                for r in range(height + 1):
                    moved = [shelf[t, pl.ds(r * pitch + 7 + TAPS[slot], width), :] for t in range(o.tiles)]
                    a[image, r + 1, :, pl.ds(slot * channels, channels)] = jnp.concatenate(moved, axis=1).astype(BF16)

    def convolve(a, image, weight):
        depth = a.shape[-1]
        total = None
        step = depth // 3
        for slot in range(3):
            for d in TAPS:
                lhs = a[image, d : d + height, :, pl.ds(slot * step, step)].reshape(pixels, step)
                term = jnp.dot(lhs, weight[d, slot], preferred_element_type=F32)
                total = term if total is None else total + term
        return total

    def put(target, values):
        for t in range(target.shape[0]):
            target[t] = values[:, t * LANES : (t + 1) * LANES]

    def sums(values):
        return [jnp.sum(values, axis=0, keepdims=True), jnp.sum(values * values, axis=0, keepdims=True)]

    for copy in x_waits:
        copy.wait()
    for copy in p_copies + w_copies:
        copy.start()
    rows0 = []
    for image in range(images):
        values = xv[image].reshape(pixels, xv.shape[-1]).astype(F32)
        put(v0.at[image], values)
        rows0.append(sums(values))
    for h in range(halves):
        local_stats(0, h, sum(rows0[h * per : (h + 1) * per], []))
        prepare_halo(0, h)
    pl.semaphore_wait(barrier, (2 * reach + 1) * nrow - 1)
    send_between(0, range(halves), reach, 1)
    for h in range(halves):
        stat_to(0, h, z, oc)
        for copy in halo_copies(0, h):
            copy.start()

    for copy in p_copies:
        copy.wait()
    w_waits[0].wait()
    for image in range(images):
        put(short.at[image], jnp.dot(
            xv[image].reshape(pixels, xv.shape[-1]), sw[...], preferred_element_type=F32) + short_bias[...])

    for h in range(halves):
        wait_stats(0, h)

    @pl.when(c == nrow - 1)
    def _():
        relay()

    last = 2 * RESNETS - 1
    for k in range(2 * RESNETS):
        if k == 0:
            a, gain, shift, weight, bias = a1, gain_in, shift_in, w1, bias_first
        else:
            j = pl.ds(k - 1, 1)
            a, gain, shift, weight, bias = a2, gains.at[j], shifts.at[j], wr.at[k - 1], biases.at[j]
        w_waits[1 + k].wait()
        for h in range(halves):
            await_all(k, h)
            load(k, h, a, gain[...], shift[...])
            rows = []
            for i in range(per):
                image = h * per + i
                result = convolve(a, image, weight) + bias[...]
                if k % 2 == 1:
                    skip = short.at[image] if k == 1 else vs.at[k - 2, image]
                    result = result + jnp.concatenate([skip[t] for t in range(skip.shape[0])], axis=1)
                rounded = result.astype(BF16)
                if k == last:
                    for r in range(height):
                        outv[image, mirrored(r, height)] = rounded[r * width : (r + 1) * width]
                else:
                    values = rounded.astype(F32)
                    put(vs.at[k, image], values)
                    rows += sums(values)
            if k < last:
                local_stats(k + 1, h, rows)
                send_far(k + 1, h)
                prepare_halo(k + 1, h)
        if k < last:
            for h in range(halves):
                finish_sends(k + 1, h)

    @pl.when(c == nrow - 1)
    def _():
        for h in range(halves):
            for copy in relay_copies(h, (oc, c)):
                copy.wait_send()


def run(nblk, nrow, halves, *args):
    x = args[0]
    w1, wr = args[3], args[9]
    images, height, width, cin = x.shape
    ch = w1.shape[-1]
    per = images // halves
    stages = 2 * RESNETS
    anywhere = pl.BlockSpec(memory_space=pl.ANY)
    inside = pl.BlockSpec(memory_space=pltpu.VMEM)
    specs = [anywhere] * len(args)
    fixed = list(args)
    for j in (1, 2, 4, 6):
        fixed[j] = args[j].reshape(1, -1)

    def halo_buffers(lead, channels):
        return [
            pltpu.VMEM((*lead, halves, 2, per * height, channels), BF16),
            pltpu.VMEM((*lead, halves, 2, per * height, channels), BF16),
            pltpu.VMEM((*lead, halves, per, channels // LANES, width, LANES), F32),
            pltpu.VMEM((*lead, halves, 2, 8, channels), F32),
            pltpu.VMEM((*lead, halves, 2, 8, channels), F32),
        ]

    return pl.pallas_call(
        functools.partial(kernel, nblk, nrow, halves),
        out_shape=pltpu.VMEM((images, height, width, ch), BF16),
        in_specs=specs,
        out_specs=inside,
        scratch_shapes=[
            *[pltpu.VMEM(fixed[j].shape, F32) for j in (1, 2, 4, 6, 7, 8, 10)],
            pltpu.VMEM((cin, LANES), BF16),
            pltpu.VMEM((ch, LANES), BF16),
            pltpu.VMEM((LANES, cin), BF16),
            pltpu.VMEM((LANES, ch), BF16),
            pltpu.VMEM(x.shape, BF16),
            pltpu.VMEM(w1.shape, BF16),
            pltpu.VMEM(wr.shape, BF16),
            pltpu.VMEM((cin, ch), BF16),
            pltpu.VMEM((images, cin // LANES, height * width, LANES), F32),
            pltpu.VMEM((stages - 1, images, ch // LANES, height * width, LANES), F32),
            pltpu.VMEM((images, ch // LANES, height * width, LANES), F32),
            pltpu.VMEM((per, cin // LANES, (height + 1) * (width + 16), LANES), F32),
            pltpu.VMEM((per, ch // LANES, (height + 1) * (width + 16), LANES), F32),
            pltpu.VMEM((images, height + 2, width, 3 * cin), BF16),
            pltpu.VMEM((images, height + 2, width, 3 * ch), BF16),
            *halo_buffers((), cin),
            *halo_buffers((stages - 1,), ch),
            pltpu.VMEM((stages, halves, 8, LANES), F32),
            pltpu.VMEM((stages, halves, nblk * nrow, LANES), F32),
            pltpu.VMEM((halves, 2, 8, LANES), F32),
            pltpu.VMEM((halves, 2, 8, LANES), F32),
            pltpu.SemaphoreType.DMA((images,)),
            pltpu.SemaphoreType.DMA((1 + stages,)),
            pltpu.SemaphoreType.DMA((7,)),
            pltpu.SemaphoreType.DMA((halves, 2, 2)),
            pltpu.SemaphoreType.DMA((halves, 2)),
            pltpu.SemaphoreType.DMA((stages, halves)),
            pltpu.SemaphoreType.DMA((stages, halves)),
            pltpu.SemaphoreType.DMA((stages, halves, 5)),
            pltpu.SemaphoreType.DMA((stages, halves, 2)),
            pltpu.SemaphoreType.DMA((stages, halves)),
            pltpu.SemaphoreType.DMA((stages, halves, 2)),
        ],
        compiler_params=pltpu.CompilerParams(
            collective_id=0, has_side_effects=True, vmem_limit_bytes=60 * 1024 * 1024),
    )(*fixed)


def solution(mesh):
    placed = (P("groups", "rows", "blk", None),) + (P(),) * 10
    return jax.shard_map(
        functools.partial(run, mesh.shape["blk"], mesh.shape["rows"], 2),
        mesh=mesh,
        in_specs=placed,
        out_specs=P("groups", "rows", "blk", None),
        check_vma=False,
    )
```

```python
import functools

import jax
import jax.numpy as jnp
from jax import lax
from jax.experimental import pallas as pl
from jax.experimental.pallas import tpu as pltpu
from jax.sharding import PartitionSpec as P

GROUPS = 32
RESNETS = 3
EPS = 1e-06
LANES = 128
TAPS = (1, 0, 2)
MESH = pl.DeviceIdType.MESH
F32 = jnp.float32
BF16 = jnp.bfloat16


def iota(shape, dim):
    return lax.broadcasted_iota(jnp.int32, shape, dim)


def three_parts(values, part):
    high = values.astype(BF16)
    rest = values - high.astype(F32)
    middle = rest.astype(BF16)
    low = (rest - middle.astype(F32)).astype(BF16)
    picked = jnp.where(part == 0, high.astype(F32), jnp.where(part == 1, middle.astype(F32), low.astype(F32)))
    return jnp.where(part < 3, picked, 0.0).astype(BF16)


def gather_matrix(channels):
    shape = (channels, LANES)
    return (iota(shape, 0) // (channels // GROUPS) == iota(shape, 1) % GROUPS).astype(F32).astype(BF16)


def spread_matrix(channels):
    shape = (LANES, channels)
    return (iota(shape, 0) % GROUPS == iota(shape, 1) // (channels // GROUPS)).astype(F32).astype(BF16)


def kernel(
    nblk,
    nrow,
    halves,
    x_hbm,
    gain_in_hbm,
    shift_in_hbm,
    w1_hbm,
    bias_first_hbm,
    sw_hbm,
    short_bias_hbm,
    gains_hbm,
    shifts_hbm,
    wr_hbm,
    biases_hbm,
    outv,
    gain_in,
    shift_in,
    bias_first,
    short_bias,
    gains,
    shifts,
    biases,
    gather1,
    gather2,
    spread1,
    spread2,
    xv,
    w1,
    wr,
    sw,
    v0,
    vs,
    short,
    s1,
    s2,
    a1,
    a2,
    col_s1,
    col_r1,
    row_r1,
    cor_s1,
    cor_r1,
    col_s2,
    col_r2,
    row_r2,
    cor_s2,
    cor_r2,
    stat_s,
    stat_r,
    relay_s,
    relay_r,
    x_sem,
    w_sem,
    p_sem,
    relay_ssem,
    relay_rsem,
    stat_ssem,
    stat_rsem,
    halo_ssem,
    colr_sem,
    rowr_sem,
    corr_sem,
):
    images, height, width, _ = xv.shape
    per = images // halves
    slots = 2 * per
    pixels = height * width
    z = lax.axis_index("blk")
    c = lax.axis_index("rows")
    oc = 1 - c
    right = lax.rem(z + 1, nblk)
    left = lax.rem(z + nblk - 1, nblk)
    me = z * nrow + c
    edge = height - 1

    def mirrored(row, rows):
        return row + c * (rows - 1 - 2 * row)


    half_way = nblk // 2
    reach = -(-half_way // 3)
    leap = half_way - reach

    def at(offset):
        return lax.rem(z + nblk + offset, nblk)

    barrier = pltpu.get_barrier_semaphore()

    def greet(i, carry):
        d = reach - i
        for zz in (at(d), at(-d)):
            for cc in (c, oc):
                pl.semaphore_signal(barrier, 1, device_id={"blk": zz, "rows": cc}, device_id_type=MESH)
        return carry

    lax.fori_loop(0, reach, greet, 0)
    pl.semaphore_signal(barrier, 1, device_id={"rows": oc}, device_id_type=MESH)

    x_waits = [pltpu.make_async_copy(x_hbm.at[i], xv.at[i], x_sem.at[i]) for i in range(images)]
    x_copies = [
        pltpu.make_async_copy(x_hbm.at[i, mirrored(r, height)], xv.at[i, r], x_sem.at[i])
        for i in range(images) for r in range(height)
    ]
    kernels = [(w1_hbm, w1)] + [(wr_hbm.at[i], wr.at[i]) for i in range(wr_hbm.shape[0])]
    w_waits = [pltpu.make_async_copy(sw_hbm, sw, w_sem.at[0])]
    w_copies = [w_waits[0]]
    for i, (source, target) in enumerate(kernels):
        w_waits.append(pltpu.make_async_copy(source, target, w_sem.at[1 + i]))
        for slot, tap in enumerate(TAPS):
            for d in range(3):
                w_copies.append(pltpu.make_async_copy(source.at[mirrored(d, 3), tap], target.at[d, slot], w_sem.at[1 + i]))
    p_copies = [
        pltpu.make_async_copy(source, target, p_sem.at[i])
        for i, (source, target) in enumerate((
            (gain_in_hbm, gain_in), (shift_in_hbm, shift_in), (bias_first_hbm, bias_first), (short_bias_hbm, short_bias),
            (gains_hbm, gains), (shifts_hbm, shifts), (biases_hbm, biases)))
    ]
    for copy in x_copies:
        copy.start()

    gather1[...] = gather_matrix(gather1.shape[0])
    gather2[...] = gather_matrix(gather2.shape[0])
    spread1[...] = spread_matrix(spread1.shape[1])
    spread2[...] = spread_matrix(spread2.shape[1])
    for a in (a1, a2):
        for i in range(images):
            a[i, 0] = jnp.zeros(a.shape[2:], BF16)

    def local_stats(k, h, rows):
        channels = rows[0].shape[1]
        which = iota((16, channels), 0)
        base = jnp.broadcast_to(rows[0], (16, channels))
        for j in range(1, slots):
            base = jnp.where(which % slots == j, rows[j], base)
        lhs = three_parts(base, which // slots)
        dots = jnp.dot(lhs, (gather1 if k == 0 else gather2)[...], preferred_element_type=F32)
        slot_of_row = iota((16, LANES), 0) % slots
        slot_of_lane = iota((16, LANES), 1) // GROUPS
        packed = jnp.sum(jnp.where(slot_of_row == slot_of_lane, dots, 0.0), axis=0, keepdims=True)
        stat_s[k, h] = jnp.broadcast_to(packed, (8, LANES))

    def stat_to(k, h, zz, cc):
        pltpu.make_async_remote_copy(
            stat_s.at[k, h, pl.ds(0, 1)], stat_r.at[k, h, pl.ds(me, 1)], stat_ssem.at[k, h], stat_rsem.at[k, h],
            device_id={"blk": zz, "rows": cc}, device_id_type=MESH,
        ).start()

    def send_between(k, hs, high, low):
        def step(i, carry):
            d = high - i
            for h in hs:
                for zz in (at(d), at(-d)):
                    for cc in range(nrow):
                        stat_to(k, h, zz, cc)
            return carry

        if high >= low:
            lax.fori_loop(0, high - low + 1, step, 0)

    def far_from(k, h):
        return (3 * half_way // 4 if k == 1 and h == 0 else 2 * half_way // 3) + 1

    def send_far(k, h):
        for cc in range(nrow):
            stat_to(k, h, at(half_way), cc)
        send_between(k, (h,), half_way - 1, far_from(k, h))

    def send_near(k, h):
        send_between(k, (h,), min(far_from(k, h), half_way) - 1, 1)
        stat_to(k, h, z, oc)

    def wait_stats(k, h):
        count = (2 * reach + 1 if k == 0 else nblk) * nrow - 1
        copy = pltpu.make_async_remote_copy(
            stat_r.at[k, h, pl.ds(0, count)], stat_r.at[k, h, pl.ds(0, count)],
            stat_ssem.at[k, h], stat_rsem.at[k, h], device_id={"rows": oc}, device_id_type=MESH,
        )
        copy.wait_send()
        copy.wait_recv()

    def gathered(k, h):
        own = iota((nblk * nrow, LANES), 0) == me
        return jnp.where(own, stat_s[k, h, 0:1], stat_r[k, h])

    def between(low, high):
        chip = iota((nblk * nrow, LANES), 0) // nrow
        return lax.rem(chip + 2 * nblk - z - low, nblk) <= high - low

    def relay_copies(h, cores):
        copies = []
        for side, zz in enumerate((at(-leap), at(leap))):
            for i, cc in enumerate(cores):
                copies.append(pltpu.make_async_remote_copy(
                    relay_s.at[h, side, pl.ds(0, 1)], relay_r.at[h, side, pl.ds(0, 1)], relay_ssem.at[h, side, i], relay_rsem.at[h, side],
                    device_id={"blk": zz, "rows": cc}, device_id_type=MESH))
        return copies

    def relay():
        for h in range(halves):
            everything = gathered(0, h)
            for side, (low, high) in enumerate(((reach + 1 - leap, reach), (1 - reach, leap - reach - 1))):
                part = jnp.sum(jnp.where(between(low, high), everything, 0.0), axis=0, keepdims=True)
                relay_s[h, side] = jnp.broadcast_to(part, (8, LANES))
        for h in range(halves):
            for copy in relay_copies(h, (oc, c)):
                copy.start()

    def relay_wait(h):
        for copy in relay_copies(h, (oc,)):
            copy.wait_recv()

    def scales(k, h, channels, gain, shift):
        count = pixels * nblk * nrow * (channels // GROUPS)
        everything = gathered(k, h)
        if k == 0:
            everything = jnp.where(between(-reach, reach), everything, 0.0)
        total = jnp.sum(everything, axis=0, keepdims=True)
        if k == 0:
            total = total + relay_r[h, 0, 0:1] + relay_r[h, 1, 0:1]
        row = iota((16, LANES), 0)
        stat = jnp.where(iota((16, LANES), 1) // GROUPS == row % slots, total * (1.0 / count), 0.0)
        lhs = three_parts(stat, row // slots)
        dots = jnp.dot(lhs, (spread1 if k == 0 else spread2)[...], preferred_element_type=F32)
        pick = lambda j: dots[j : j + 1] + dots[slots + j : slots + j + 1] + dots[2 * slots + j : 2 * slots + j + 1]
        result = []
        for i in range(per):
            center = pick(2 * i)
            a = lax.rsqrt(jnp.maximum(pick(2 * i + 1) - center * center, 0.0) + EPS) * gain
            result.append((0.5 * a, 0.5 * (shift - center * a)))
        return result

    def activate(values, ab):
        half = values * ab[0] + ab[1]
        return half + half * jnp.tanh(half)

    class Halo:
        pass

    def halo_of(k):
        o = Halo()
        first = k == 0
        o.v = v0 if first else vs.at[k - 1]
        o.col_s = col_s1 if first else col_s2.at[k - 1]
        o.col_r = col_r1 if first else col_r2.at[k - 1]
        o.row_r = row_r1 if first else row_r2.at[k - 1]
        o.cor_s = cor_s1 if first else cor_s2.at[k - 1]
        o.cor_r = cor_r1 if first else cor_r2.at[k - 1]
        o.tiles = o.v.shape[1]
        o.channels = o.tiles * LANES
        return o

    def halo_copies(k, h):
        o = halo_of(k)
        copies = []
        for side, (near, blk) in enumerate(((0, right), (1, left))):
            copies.append(pltpu.make_async_remote_copy(
                o.col_s.at[h, side], o.col_r.at[h, side], halo_ssem.at[k, h, 2 * side], colr_sem.at[k, h, side],
                device_id={"blk": blk, "rows": c}, device_id_type=MESH))
            copies.append(pltpu.make_async_remote_copy(
                o.cor_s.at[h, side, pl.ds(0, per)], o.cor_r.at[h, side, pl.ds(0, per)], halo_ssem.at[k, h, 2 * side + 1], corr_sem.at[k, h, side],
                device_id={"blk": blk, "rows": oc}, device_id_type=MESH))
        copies.append(pltpu.make_async_remote_copy(
            o.v.at[pl.ds(h * per, per), :, pl.ds(edge * width, width)], o.row_r.at[h], halo_ssem.at[k, h, 4], rowr_sem.at[k, h],
            device_id={"rows": oc}, device_id_type=MESH))
        return copies

    def prepare_halo(k, h):
        o = halo_of(k)
        for side in range(2):
            q = width - 1 if side == 0 else 0
            for t in range(o.tiles):
                lanes = pl.ds(t * LANES, LANES)
                cols = [o.v[h * per + i, t, pl.ds(q, height, stride=width), :] for i in range(per)]
                o.col_s[h, side, :, lanes] = jnp.concatenate(cols, axis=0).astype(BF16)
                corner = edge * width + q
                block = jnp.zeros((8, LANES), F32)
                for i in range(per):
                    around = o.v[h * per + i, t, pl.ds(corner // 8 * 8, 8), :]
                    block = jnp.where(iota((8, LANES), 0) == i, around[corner % 8 : corner % 8 + 1], block)
                o.cor_s[h, side, :, lanes] = block

    def finish_sends(k):
        for h in range(halves):
            send_near(k, h)
        for h in range(halves):
            for copy in halo_copies(k, h):
                copy.start()

    def await_all(k, h):
        for copy in halo_copies(k, h):
            copy.wait()
        if k == 0:
            relay_wait(h)
        else:
            wait_stats(k, h)

    def load(k, h, a, gain, shift):
        o = halo_of(k)
        channels = o.channels
        factors = scales(k, h, channels, gain, shift)
        pitch = width + 16
        for i in range(per):
            image = h * per + i
            shelf = (s1 if k == 0 else s2).at[i]
            tiles = [slice(t * LANES, (t + 1) * LANES) for t in range(o.tiles)]
            ab = [[x[:, t] for x in factors[i]] for t in tiles]

            for s, at_column in enumerate((7, width + 8)):
                for t, lanes in enumerate(tiles):
                    side = activate(o.col_r[h, s, pl.ds(i * height, height), lanes].astype(F32), ab[t])
                    shelf[t, pl.ds(at_column, height, stride=pitch), :] = side
                    shelf[t, pl.ds(height * pitch + at_column, 1), :] = activate(o.cor_r[h, s, :, lanes][i : i + 1], ab[t])
            for r in range(height + 1):
                center = []
                for t in range(o.tiles):
                    source = o.v[image, t, pl.ds(r * width, width), :] if r < height else o.row_r[h, i, t]
                    act = activate(source, ab[t])
                    shelf[t, pl.ds(r * pitch + 8, width), :] = act
                    center.append(act)
                a[image, r + 1, :, pl.ds(0, channels)] = jnp.concatenate(center, axis=1).astype(BF16)
            for slot in (1, 2):
                for r in range(height + 1):
                    moved = [shelf[t, pl.ds(r * pitch + 7 + TAPS[slot], width), :] for t in range(o.tiles)]
                    a[image, r + 1, :, pl.ds(slot * channels, channels)] = jnp.concatenate(moved, axis=1).astype(BF16)

    def convolve(a, image, weight):
        depth = a.shape[-1]
        total = None
        step = depth // 3
        for slot in range(3):
            for d in TAPS:
                lhs = a[image, d : d + height, :, pl.ds(slot * step, step)].reshape(pixels, step)
                term = jnp.dot(lhs, weight[d, slot], preferred_element_type=F32)
                total = term if total is None else total + term
        return total

    def put(target, values):
        for t in range(target.shape[0]):
            target[t] = values[:, t * LANES : (t + 1) * LANES]

    def sums(values):
        return [jnp.sum(values, axis=0, keepdims=True), jnp.sum(values * values, axis=0, keepdims=True)]

    for copy in x_waits:
        copy.wait()
    for copy in p_copies + w_copies:
        copy.start()
    rows0 = []
    for image in range(images):
        values = xv[image].reshape(pixels, xv.shape[-1]).astype(F32)
        put(v0.at[image], values)
        rows0.append(sums(values))
    for h in range(halves):
        local_stats(0, h, sum(rows0[h * per : (h + 1) * per], []))
        prepare_halo(0, h)
    pl.semaphore_wait(barrier, (2 * reach + 1) * nrow - 1)
    send_between(0, range(halves), reach, 1)
    for h in range(halves):
        stat_to(0, h, z, oc)
        for copy in halo_copies(0, h):
            copy.start()

    for copy in p_copies:
        copy.wait()
    w_waits[0].wait()
    for image in range(images):
        put(short.at[image], jnp.dot(
            xv[image].reshape(pixels, xv.shape[-1]), sw[...], preferred_element_type=F32) + short_bias[...])

    for h in range(halves):
        wait_stats(0, h)

    @pl.when(c == nrow - 1)
    def _():
        relay()

    last = 2 * RESNETS - 1
    for k in range(2 * RESNETS):
        if k == 0:
            a, gain, shift, weight, bias = a1, gain_in, shift_in, w1, bias_first
        else:
            j = pl.ds(k - 1, 1)
            a, gain, shift, weight, bias = a2, gains.at[j], shifts.at[j], wr.at[k - 1], biases.at[j]
        w_waits[1 + k].wait()
        for h in range(halves):
            await_all(k, h)
            load(k, h, a, gain[...], shift[...])
            rows = []
            for i in range(per):
                image = h * per + i
                result = convolve(a, image, weight) + bias[...]
                if k % 2 == 1:
                    skip = short.at[image] if k == 1 else vs.at[k - 2, image]
                    result = result + jnp.concatenate([skip[t] for t in range(skip.shape[0])], axis=1)
                rounded = result.astype(BF16)
                if k == last:
                    for r in range(height):
                        outv[image, mirrored(r, height)] = rounded[r * width : (r + 1) * width]
                else:
                    values = rounded.astype(F32)
                    put(vs.at[k, image], values)
                    rows += sums(values)
            if k < last:
                local_stats(k + 1, h, rows)
                send_far(k + 1, h)
                prepare_halo(k + 1, h)
        if k < last:
            finish_sends(k + 1)

    @pl.when(c == nrow - 1)
    def _():
        for h in range(halves):
            for copy in relay_copies(h, (oc, c)):
                copy.wait_send()


def run(nblk, nrow, halves, *args):
    x = args[0]
    w1, wr = args[3], args[9]
    images, height, width, cin = x.shape
    ch = w1.shape[-1]
    per = images // halves
    stages = 2 * RESNETS
    anywhere = pl.BlockSpec(memory_space=pl.ANY)
    inside = pl.BlockSpec(memory_space=pltpu.VMEM)
    specs = [anywhere] * len(args)
    fixed = list(args)
    for j in (1, 2, 4, 6):
        fixed[j] = args[j].reshape(1, -1)

    def halo_buffers(lead, channels):
        return [
            pltpu.VMEM((*lead, halves, 2, per * height, channels), BF16),
            pltpu.VMEM((*lead, halves, 2, per * height, channels), BF16),
            pltpu.VMEM((*lead, halves, per, channels // LANES, width, LANES), F32),
            pltpu.VMEM((*lead, halves, 2, 8, channels), F32),
            pltpu.VMEM((*lead, halves, 2, 8, channels), F32),
        ]

    return pl.pallas_call(
        functools.partial(kernel, nblk, nrow, halves),
        out_shape=pltpu.VMEM((images, height, width, ch), BF16),
        in_specs=specs,
        out_specs=inside,
        scratch_shapes=[
            *[pltpu.VMEM(fixed[j].shape, F32) for j in (1, 2, 4, 6, 7, 8, 10)],
            pltpu.VMEM((cin, LANES), BF16),
            pltpu.VMEM((ch, LANES), BF16),
            pltpu.VMEM((LANES, cin), BF16),
            pltpu.VMEM((LANES, ch), BF16),
            pltpu.VMEM(x.shape, BF16),
            pltpu.VMEM(w1.shape, BF16),
            pltpu.VMEM(wr.shape, BF16),
            pltpu.VMEM((cin, ch), BF16),
            pltpu.VMEM((images, cin // LANES, height * width, LANES), F32),
            pltpu.VMEM((stages - 1, images, ch // LANES, height * width, LANES), F32),
            pltpu.VMEM((images, ch // LANES, height * width, LANES), F32),
            pltpu.VMEM((per, cin // LANES, (height + 1) * (width + 16), LANES), F32),
            pltpu.VMEM((per, ch // LANES, (height + 1) * (width + 16), LANES), F32),
            pltpu.VMEM((images, height + 2, width, 3 * cin), BF16),
            pltpu.VMEM((images, height + 2, width, 3 * ch), BF16),
            *halo_buffers((), cin),
            *halo_buffers((stages - 1,), ch),
            pltpu.VMEM((stages, halves, 8, LANES), F32),
            pltpu.VMEM((stages, halves, nblk * nrow, LANES), F32),
            pltpu.VMEM((halves, 2, 8, LANES), F32),
            pltpu.VMEM((halves, 2, 8, LANES), F32),
            pltpu.SemaphoreType.DMA((images,)),
            pltpu.SemaphoreType.DMA((1 + stages,)),
            pltpu.SemaphoreType.DMA((7,)),
            pltpu.SemaphoreType.DMA((halves, 2, 2)),
            pltpu.SemaphoreType.DMA((halves, 2)),
            pltpu.SemaphoreType.DMA((stages, halves)),
            pltpu.SemaphoreType.DMA((stages, halves)),
            pltpu.SemaphoreType.DMA((stages, halves, 5)),
            pltpu.SemaphoreType.DMA((stages, halves, 2)),
            pltpu.SemaphoreType.DMA((stages, halves)),
            pltpu.SemaphoreType.DMA((stages, halves, 2)),
        ],
        compiler_params=pltpu.CompilerParams(
            collective_id=0, has_side_effects=True, vmem_limit_bytes=60 * 1024 * 1024),
    )(*fixed)


def solution(mesh):
    placed = (P("groups", "rows", "blk", None),) + (P(),) * 10
    return jax.shard_map(
        functools.partial(run, mesh.shape["blk"], mesh.shape["rows"], 2),
        mesh=mesh,
        in_specs=placed,
        out_specs=P("groups", "rows", "blk", None),
        check_vma=False,
    )
```
